32 devices in a mesh: dp: 8 (over z, x), zero: 4 (over y, core).
Axes of the slice: x: 2, y: 2, z: 4, core: 2. Of those that a mesh axis runs over, the one named last changes fastest.
Arguments:
- tokens: float32 [32768, 768], P(('dp', 'zero')), may hold values from -6 to 6
- cotangent: float32 [32768, 768], P(('dp', 'zero')), may hold values from -6 to 6
- lengths: int32 [32], P(('dp', 'zero')), may hold values from 0 to 1024, as said below
- master_matrix: float32 [9216, 768], P(('dp', 'zero')), may hold values from -2 to 2
- master_vector: float32 [12, 768], P(None, ('dp', 'zero')), may hold values from -2 to 2
- moment_matrix: float32 [9216, 768], P(('dp', 'zero')), may hold values from -2 to 2
- moment_vector: float32 [12, 768], P(None, ('dp', 'zero')), may hold values from -2 to 2
- square_matrix: float32 [9216, 768], P(('dp', 'zero')), may hold values from 0.01 to 0.3
- square_vector: float32 [12, 768], P(None, ('dp', 'zero')), may hold values from 0.01 to 0.3
Outputs:
- block_out: float32 [32768, 768], P(('dp', 'zero'))
- input_gradient: float32 [32768, 768], P(('dp', 'zero'))
- matrix_gradient: float32 [9216, 768], P(('dp', 'zero'))
- vector_gradient: float32 [12, 768], P(None, ('dp', 'zero'))
- matrix_weights: float32 [9216, 768], P(('dp', 'zero'))
- vector_weights: float32 [12, 768], P(None, ('dp', 'zero'))
- matrix_moment: float32 [9216, 768], P(('dp', 'zero'))
- vector_moment: float32 [12, 768], P(None, ('dp', 'zero'))
- matrix_square: float32 [9216, 768], P(('dp', 'zero'))
- vector_square: float32 [12, 768], P(None, ('dp', 'zero'))
The draws below stay inside these ranges and needn't reach their ends.
Inputs may be any that keep to these rules, and one draw needn't show every extreme that they name: A slot holds a sequence of lengths tokens from its start; 0 marks an empty slot; nonzero lengths are at least 512, and some slot has exactly 1024.
All inputs are finite; a program needn't handle non-finite values.
Results may differ from the reference program's by a relative error of at most 0.012.
Values may be sent and summed in bfloat16 or wider, within the bound.
A program may use at most 256 MiB of HBM per device.

```python
import math
import jax
import jax.numpy as jnp
from jax import lax

D = 768
HEADS = 12
HD = 64
FF = 3072
SEQ = 1024
ADAM_STEP = 2
SEQS = 32
TOKENS = 32768
MROWS = 9216
VROWS = 12


def draw_lengths(key, part):
    keep_key = jax.random.fold_in(key, 11)
    size_key = jax.random.fold_in(key, 12)
    full_key = jax.random.fold_in(key, 13)
    keep = jax.random.randint(keep_key, (SEQS,), 0, 5) > 0
    sizes = jax.random.randint(size_key, (SEQS,), SEQ // 2, SEQ + 1)
    chosen = jnp.where(keep, sizes, 0)
    where_full = jax.random.randint(full_key, (), 0, SEQS)
    slots = jnp.arange(SEQS, dtype=jnp.int32)
    return jnp.where(slots == where_full, SEQ, chosen).astype(jnp.int32)


def draw_master_matrix(key, part):
    base = jnp.clip(jax.random.normal(key, (MROWS, D), jnp.float32), -6.0, 6.0)
    rows = jnp.arange(MROWS, dtype=jnp.int32)
    narrow = float(D) ** (-0.5)
    scale = jnp.where(rows < 3 * D, narrow, jnp.where(rows < 4 * D, 8.0 * narrow, jnp.where(rows < 4 * D + FF, narrow, float(FF) ** (-0.5))))
    out = base * scale[:, None]
    return jnp.clip(out, -2.0, 2.0)


def draw_master_vector(key, part):
    base = 0.2 * jnp.clip(jax.random.normal(key, (VROWS, D), jnp.float32), -6.0, 6.0)
    gains = 1.0 + 0.6 * (jax.random.uniform(jax.random.fold_in(key, 3), (VROWS, D), jnp.float32) - 0.5)
    rows = jnp.arange(VROWS, dtype=jnp.int32)[:, None]
    return jnp.where((rows == 0) | (rows == 5), gains, base)


def shard_levels(own_key, shape, pieces, low, largest):
    def one(axis_at, blocks):
        draws = jax.random.uniform(jax.random.fold_in(jax.random.fold_in(own_key, 6), axis_at), (blocks,), jnp.float32, low / len(pieces), largest / len(pieces))
        return jnp.repeat(jnp.exp(draws), shape[axis_at] // blocks).reshape((-1,) + (1,) * (len(shape) - axis_at - 1))

    factor_of = one(*pieces[0])
    for cut in pieces[1:]:
        factor_of = factor_of * one(*cut)
    return factor_of


def normal_values(own_key, extent, deviation, most, cuts=(), kind=jnp.bfloat16):
    entries = deviation * jax.random.normal(own_key, extent, jnp.float32)
    if cuts:
        entries = entries * shard_levels(own_key, extent, cuts, -0.22, 0.18)
    return jnp.clip(entries, -most, most).astype(kind)


def setup_inputs(seed: int = 0) -> dict:
    arg_keys = jax.random.split(jax.random.key(seed), 10)
    tokens = normal_values(arg_keys[0], (TOKENS, D), 1.0, 6.0, ((0, 32),), jnp.float32)
    cotangent = normal_values(arg_keys[1], (TOKENS, D), 1.0, 6.0, ((0, 32),), jnp.float32)
    lengths = draw_lengths(jax.random.fold_in(arg_keys[9], 71), 0)
    master_matrix = draw_master_matrix(jax.random.fold_in(arg_keys[9], 71), 0)
    master_vector = draw_master_vector(jax.random.fold_in(arg_keys[9], 71), 0)
    moment_matrix = normal_values(arg_keys[5], (MROWS, D), 0.15, 2.0, ((0, 32),), jnp.float32)
    moment_vector = normal_values(arg_keys[6], (VROWS, D), 0.15, 2.0, ((1, 32),), jnp.float32)
    square_matrix = jnp.clip(jnp.exp(math.log(0.3) - 3.4011974 * jax.random.uniform(arg_keys[7], (MROWS, D), jnp.float32) ** shard_levels(arg_keys[7], (MROWS, D), ((0, 32),), -0.2, 0.2)), 0.01, 0.3)
    square_vector = jnp.clip(jnp.exp(math.log(0.3) - 3.4011974 * jax.random.uniform(arg_keys[8], (VROWS, D), jnp.float32) ** shard_levels(arg_keys[8], (VROWS, D), ((1, 32),), -0.2, 0.2)), 0.01, 0.3)
    return {"tokens": tokens, "cotangent": cotangent, "lengths": lengths, "master_matrix": master_matrix, "master_vector": master_vector, "moment_matrix": moment_matrix, "moment_vector": moment_vector, "square_matrix": square_matrix, "square_vector": square_vector}


EPS = 1e-05
NEG = -1e+30
BETA_ONE = 0.9
BETA_TWO = 0.95
ADAM_EPS = 1e-08
LR_MATRIX = 0.05
LR_VECTOR = 0.1
DECAY = 0.1
CUBIC = 0.044715
ROOT = 0.7978845608028654
GRAD_FACTOR = 4.0

def lowered(value):
    return lax.optimization_barrier(value.astype(jnp.bfloat16))

def contract_last(left, right):
    return lax.dot_general(left, right, (((1,), (1,)), ((), ())), preferred_element_type=jnp.float32)

def contract_first(left, right):
    return lax.dot_general(left, right, (((0,), (0,)), ((), ())), preferred_element_type=jnp.float32)

def norm_forward(rows, gain, shift):
    centre = lax.optimization_barrier(jnp.mean(rows, -1, keepdims=True))
    centred = rows - centre
    spread = lax.optimization_barrier(jnp.mean(centred * centred, -1, keepdims=True))
    inverse = lax.rsqrt(spread + EPS)
    unit = centred * inverse
    return ((unit * gain + shift).astype(jnp.bfloat16), unit, inverse)

def norm_backward(out_grad, gain, unit, inverse):
    scaled = out_grad * gain
    return inverse * (scaled - lax.optimization_barrier(jnp.mean(scaled, -1, keepdims=True)) - unit * lax.optimization_barrier(jnp.mean(scaled * unit, -1, keepdims=True)))

def causal(start, width, span):
    rows = start + jnp.arange(width, dtype=jnp.int32)[:, None]
    columns = jnp.arange(span, dtype=jnp.int32)[None, :]
    return columns <= rows

def attend_forward(queries, keys, values):
    width = min(512, SEQ)
    scale = float(HD) ** (-0.5)
    query_wide = queries.astype(jnp.float32)
    key_wide = keys.astype(jnp.float32)
    value_wide = values.astype(jnp.float32)
    mixed_parts = []
    logsums = []
    for start in range(0, SEQ, width):
        scores = jnp.einsum('qhd,khd->hqk', query_wide[start:start + width], key_wide) * scale
        scores = jnp.where(causal(start, width, SEQ), scores, NEG)
        top = lax.optimization_barrier(jnp.max(scores, -1, keepdims=True))
        logsum = top + jnp.log(lax.optimization_barrier(jnp.sum(jnp.exp(scores - top), -1, keepdims=True)))
        probs = lowered(jnp.exp(scores - logsum)).astype(jnp.float32)
        mixed_parts.append(jnp.einsum('hqk,khd->qhd', probs, value_wide))
        logsums.append(logsum)
    mixed = jnp.concatenate(mixed_parts, 0).astype(jnp.bfloat16)
    return (mixed, logsums)

def attend_backward(queries, keys, values, mixed, logsums, mixed_grad):
    width = min(512, SEQ)
    scale = float(HD) ** (-0.5)
    query_wide = queries.astype(jnp.float32)
    key_wide = keys.astype(jnp.float32)
    value_wide = values.astype(jnp.float32)
    grad_wide = mixed_grad.astype(jnp.float32)
    delta = lax.optimization_barrier(jnp.sum(grad_wide * mixed.astype(jnp.float32), -1))
    key_total = jnp.zeros(keys.shape, jnp.float32)
    value_total = jnp.zeros(values.shape, jnp.float32)
    query_parts = []
    for index, start in enumerate(range(0, SEQ, width)):
        query_block = query_wide[start:start + width]
        grad_block = grad_wide[start:start + width]
        scores = jnp.einsum('qhd,khd->hqk', query_block, key_wide) * scale
        scores = jnp.where(causal(start, width, SEQ), scores, NEG)
        probs = jnp.exp(scores - logsums[index])
        prob_low = lowered(probs).astype(jnp.float32)
        value_total = value_total + jnp.einsum('hqk,qhd->khd', prob_low, grad_block)
        dprob = jnp.einsum('qhd,khd->hqk', grad_block, value_wide)
        dscore = probs * (dprob - jnp.transpose(delta[start:start + width])[:, :, None])
        score_low = lowered(dscore).astype(jnp.float32)
        query_parts.append(jnp.einsum('hqk,khd->qhd', score_low, key_wide) * scale)
        key_total = key_total + jnp.einsum('hqk,qhd->khd', score_low, query_block) * scale
    return (jnp.concatenate(query_parts, 0), key_total, value_total)

def layer_pass(rows, cotangent, length, weights, vectors):
    w_qkv = weights[:3 * D]
    w_out = weights[3 * D:4 * D]
    w_fc = weights[4 * D:4 * D + FF]
    w_down = weights[4 * D + FF:]
    bias_fc = vectors[8:].reshape(FF)
    live = (jnp.arange(SEQ, dtype=jnp.int32) < length).astype(jnp.float32)[:, None]
    normed_one, unit_one, inverse_one = norm_forward(rows, vectors[0], vectors[1])
    projected = contract_last(normed_one, w_qkv)
    queries = (projected[:, :D] + vectors[2]).astype(jnp.bfloat16).reshape(SEQ, HEADS, HD)
    keys = projected[:, D:2 * D].astype(jnp.bfloat16).reshape(SEQ, HEADS, HD)
    values = (projected[:, 2 * D:] + vectors[3]).astype(jnp.bfloat16).reshape(SEQ, HEADS, HD)
    mixed, logsums = attend_forward(queries, keys, values)
    mixed_flat = mixed.reshape(SEQ, D)
    after_attention = rows + contract_last(mixed_flat, w_out) + vectors[4]
    normed_two, unit_two, inverse_two = norm_forward(after_attention, vectors[5], vectors[6])
    hidden = contract_last(normed_two, w_fc) + bias_fc
    bent = jnp.tanh(ROOT * (hidden + CUBIC * hidden * hidden * hidden))
    active = (0.5 * hidden * (1.0 + bent)).astype(jnp.bfloat16)
    result = after_attention + jnp.dot(active, w_down, preferred_element_type=jnp.float32) + vectors[7]
    block_out = jnp.where(live > 0, result, rows)
    top_grad = cotangent * live
    top_low = top_grad.astype(jnp.bfloat16)
    grad_down = contract_first(active, top_low)
    active_grad = contract_last(top_low, w_down)
    slope = 0.5 * (1.0 + bent) + 0.5 * hidden * (1.0 - bent * bent) * ROOT * (1.0 + 3.0 * CUBIC * hidden * hidden)
    hidden_grad = active_grad * slope
    hidden_low = hidden_grad.astype(jnp.bfloat16)
    grad_fc = contract_first(hidden_low, normed_two)
    normed_two_grad = jnp.dot(hidden_low, w_fc, preferred_element_type=jnp.float32)
    mid_grad = top_grad + norm_backward(normed_two_grad, vectors[5], unit_two, inverse_two)
    mid_low = mid_grad.astype(jnp.bfloat16)
    grad_out = contract_first(mid_low, mixed_flat)
    mixed_grad = jnp.dot(mid_low, w_out, preferred_element_type=jnp.float32).astype(jnp.bfloat16)
    query_grad, key_grad, value_grad = attend_backward(queries, keys, values, mixed, logsums, mixed_grad.reshape(SEQ, HEADS, HD))
    query_grad = query_grad.reshape(SEQ, D)
    key_grad = key_grad.reshape(SEQ, D)
    value_grad = value_grad.reshape(SEQ, D)
    projected_low = jnp.concatenate([query_grad, key_grad, value_grad], 1).astype(jnp.bfloat16)
    grad_qkv = contract_first(projected_low, normed_one)
    normed_one_grad = jnp.dot(projected_low, w_qkv, preferred_element_type=jnp.float32)
    input_gradient = mid_grad + norm_backward(normed_one_grad, vectors[0], unit_one, inverse_one) + (1.0 - live) * cotangent
    matrix_sum = jnp.concatenate([grad_qkv, grad_out, grad_fc, grad_down], 0)
    vector_sum = jnp.concatenate([jnp.stack([lax.optimization_barrier(jnp.sum(normed_one_grad * unit_one, 0)), lax.optimization_barrier(jnp.sum(normed_one_grad, 0)), lax.optimization_barrier(jnp.sum(query_grad, 0)), lax.optimization_barrier(jnp.sum(value_grad, 0)), lax.optimization_barrier(jnp.sum(mid_grad, 0)), lax.optimization_barrier(jnp.sum(normed_two_grad * unit_two, 0)), lax.optimization_barrier(jnp.sum(normed_two_grad, 0)), lax.optimization_barrier(jnp.sum(top_grad, 0))], 0), lax.optimization_barrier(jnp.sum(hidden_grad, 0)).reshape(FF // D, D)], 0)
    return (block_out, input_gradient, matrix_sum, vector_sum)

def adamw(master, gradient, moment, square, rate, decay):
    moment_new = BETA_ONE * moment + (1.0 - BETA_ONE) * gradient
    square_new = BETA_TWO * square + (1.0 - BETA_TWO) * gradient * gradient
    first_fix = 1.0 - BETA_ONE ** ADAM_STEP
    second_fix = 1.0 - BETA_TWO ** ADAM_STEP
    stride = moment_new / first_fix / (jnp.sqrt(square_new / second_fix) + ADAM_EPS)
    return (master - rate * (stride + decay * master), moment_new, square_new)

def reference(tokens, cotangent, lengths, master_matrix, master_vector, moment_matrix, moment_vector, square_matrix, square_vector):
    weights = master_matrix.astype(jnp.bfloat16)
    vectors = lowered(master_vector).astype(jnp.float32)
    rows_all = tokens.reshape(SEQS, SEQ, D)
    cot_all = cotangent.reshape(SEQS, SEQ, D)

    def one_sequence(carry, inputs):
        matrix_total, vector_total = carry
        out_rows, in_grad, matrix_part, vector_part = layer_pass(inputs[0], inputs[1], inputs[2], weights, vectors)
        return ((matrix_total + matrix_part, vector_total + vector_part), (out_rows, in_grad))
    start = (jnp.zeros((MROWS, D), jnp.float32), jnp.zeros((VROWS, D), jnp.float32))
    totals, outputs = lax.scan(one_sequence, start, (rows_all, cot_all, lengths))
    scale = GRAD_FACTOR * float(TOKENS) ** (-0.5)
    matrix_gradient = totals[0] * scale
    vector_gradient = totals[1] * scale
    matrix_weights, matrix_moment, matrix_square = adamw(master_matrix, matrix_gradient, moment_matrix, square_matrix, LR_MATRIX, DECAY)
    vector_weights, vector_moment, vector_square = adamw(master_vector, vector_gradient, moment_vector, square_vector, LR_VECTOR, 0.0)
    block_out = outputs[0].reshape(TOKENS, D)
    input_gradient = outputs[1].reshape(TOKENS, D)
    return (block_out, input_gradient, matrix_gradient, vector_gradient, matrix_weights, vector_weights, matrix_moment, vector_moment, matrix_square, vector_square)
```

```python
import functools
import jax, jax.numpy as jnp
from jax import lax
from jax.experimental import pallas as pl
from jax.experimental.pallas import tpu as pltpu
from jax.sharding import PartitionSpec as P

f32, bf16 = jnp.float32, jnp.bfloat16
D = 768
SEQ = 1024
PAIRS = 6
FF = 3072
EPS = 1e-05
NEG = -1e30
CUBIC = 0.044715
ROOT = 0.7978845608028654
QB = 256
NT = (((1,), (1,)), ((), ()))
NN = (((1,), (0,)), ((), ()))
TN = (((0,), (0,)), ((), ()))


def dot(a, b, dn):
    return lax.dot_general(a, b, dn, preferred_element_type=f32)


def cuts(rows, parts):
    marks = [8 * round(rows * h / parts / 8) for h in range(parts + 1)]
    return [(marks[h], marks[h + 1] - marks[h]) for h in range(parts)]


class Place:
    def __init__(self, n_dp):
        self.na = n_dp // 2
        dp, zero = lax.axis_index("dp"), lax.axis_index("zero")
        self.a, self.b, self.y, self.c = dp // 2, dp % 2, zero // 2, zero % 2

    def sid(self, a, b, y, c):
        return ((a * 2 + b) * 2 + y) * 2 + c

    def dev(self, a, b, y, c):
        return {"dp": a * 2 + b, "zero": y * 2 + c}

    def x_mate(self):
        return self.dev(self.a, 1 - self.b, self.y, self.c)

    def y_mate(self):
        return self.dev(self.a, self.b, 1 - self.y, self.c)

    def core_mate(self):
        return self.dev(self.a, self.b, self.y, 1 - self.c)

    def at(self, a):
        return self.dev(a, self.b, self.y, self.c)


def greet(me):
    barrier = pltpu.get_barrier_semaphore()
    for peer in (me.x_mate(), me.y_mate(), me.core_mate()):
        pl.semaphore_signal(barrier, inc=1, device_id=peer)
    for i in range(1, me.na):
        pl.semaphore_signal(barrier, inc=1, device_id=me.at((me.a + i) % me.na))
    pl.semaphore_wait(barrier, me.na + 2)


FINE = 4
HALVES = 2


def forward_kernel(
    n_dp, lengths, tokens_in, master_in, vector_in, cot_in,
    whole, ge, n1_out, qkv_out, mixed_out, low_out, base_out, block_out, vec, lse, part_sums,
    tokens, master, vector, cot, load_sem, save_sem,
    n1, qkv, mixed, low, after, acc, ngrad, n2, top_low, act, hid, w_out, wf, wd, w_sem, stage, stage_sem,
    own, own_sem, wq, wq_sem, tile, tiles_in, vin, vtmp, vs_sem, vr_sem, lc,
    ch_s, ch_r, up_s, dn_s, ds, xs, xr, ys, yr, fs, fr, ks, kr,
):
    me = Place(n_dp)
    na = me.na
    nq = na // 4
    a, b, y, c = me.a, me.b, me.y, me.c
    rows = master.shape[0]
    relay = na == 4
    around = ((b, y), (1 - b, y), (b, 1 - y), (1 - b, 1 - y))

    def remote(s, h, n, send, recv, peer):
        first, size = cuts(rows, n)[h]
        ref = whole.at[pl.ds(pl.multiple_of(s * rows + first, 8), size)]
        return pltpu.make_async_remote_copy(
            src_ref=ref, dst_ref=ref, send_sem=send, recv_sem=recv, device_id=peer
        )

    def chain_down(a_, h):
        return remote(me.sid(a_, b, y, c), h, FINE, ch_s.at[a_, h], ch_r.at[a_, h], me.at(a - 1))

    def chain_up(a_, h):
        return remote(me.sid(a_, b, y, c), h, FINE, ch_s.at[na + a_, h], ch_r.at[a_, h], me.at(a + 1))

    def direct(to):
        return remote(me.sid(a, b, y, c), 0, 1, ds.at[to], ch_r.at[a, 0], me.at(to))

    def direct_from(a_):
        return remote(me.sid(a_, b, y, c), 0, 1, ds.at[a_], ch_r.at[a_, 0], me.at(a_))

    def x_copy(a_, h, n, mine=True):
        return remote(me.sid(a_, b if mine else 1 - b, y, c), h, n, xs.at[a_, h], xr.at[a_, h], me.x_mate())

    def y_copy(a_, h, n, mine=True):
        return remote(me.sid(a_, b, y if mine else 1 - y, c), h, n, ys.at[a_, h], yr.at[a_, h], me.y_mate())

    def diag_send(a_, h, n):
        if h < n // 2:
            return remote(me.sid(a_, 1 - b, y, c), h, n, fs.at[a_, h], fr.at[a_, h], me.y_mate())
        return remote(me.sid(a_, b, 1 - y, c), h, n, fs.at[a_, h], fr.at[a_, h], me.x_mate())

    def diag_recv(a_, h, n):
        return remote(me.sid(a_, 1 - b, 1 - y, c), h, n, fs.at[a_, h], fr.at[a_, h], me.x_mate())

    def core(a_, b_, y_, h, n, mine=True):
        o = (b_ + b) % 2 + 2 * ((y_ + y) % 2)
        return remote(
            me.sid(a_, b_, y_, c if mine else 1 - c), h, n, ks.at[a_, o, h], kr.at[a_, o, h], me.core_mate()
        )

    def column_sends(a_, h, n):
        x_copy(a_, h, n).start()
        y_copy(a_, h, n).start()
        core(a_, b, y, h, n).start()

    def pass_chain(h):
        for a_ in range(nq):
            @pl.when(a != a_)
            def _():
                chain_up(a_, h).wait_recv()

                @pl.when((a_ < a) & (a + 1 < na))
                def _():
                    chain_up(a_, h).start()

                @pl.when((a_ > a) & (a > 0))
                def _():
                    chain_down(a_, h).start()

                column_sends(a_, h, FINE)

    def relay_up(a_):
        return remote(me.sid(a_, b, y, c), 0, 1, up_s.at[a_], ch_r.at[a_, 0], me.at(a + 1))

    def relay_down(a_):
        return remote(me.sid(a_, b, y, c), 0, 1, dn_s.at[a_], ch_r.at[a_, 0], me.at(a - 1))

    def take(a_):
        direct_from(a_).wait_recv()
        if relay:
            @pl.when((a_ < a) & (a + 1 < na))
            def _():
                relay_up(a_).start()

            @pl.when((a_ > a) & (a > 0))
            def _():
                relay_down(a_).start()

    def take_at(k):
        a_ = a + k

        @pl.when((a_ >= nq) & (a_ < na))
        def _():
            take(a_)

    def share(a_):
        for h in range(HALVES):
            column_sends(a_, h, HALVES)

    def pass_plane(a_, n):
        for h in range(n):
            x_copy(a_, h, n, False).wait_recv()
            if h < n // 2:
                diag_send(a_, h, n).start()
            core(a_, 1 - b, y, h, n).start()
            y_copy(a_, h, n, False).wait_recv()
            if h >= n // 2:
                diag_send(a_, h, n).start()
            core(a_, b, 1 - y, h, n).start()

    def pass_diag(a_, n):
        for h in range(n):
            diag_recv(a_, h, n).wait_recv()
            core(a_, 1 - b, 1 - y, h, n).start()

    def partner(a_, n):
        for b_, y_ in around:
            for h in range(n):
                core(a_, b_, y_, h, n, False).wait_recv()

    def load(k, src, dst):
        return pltpu.make_async_copy(src, dst, load_sem.at[k])

    loads = [load(0, master_in, master), load(1, vector_in, vector), load(2, tokens_in, tokens), load(3, cot_in, cot)]
    for one in loads:
        one.start()
    mine = me.sid(a, b, y, c)
    columns = vector.shape[1]
    loads[0].wait()
    loads[1].wait()
    own[...] = master[...].astype(bf16)
    put = pltpu.make_async_copy(own, whole.at[pl.ds(pl.multiple_of(mine * rows, 8), rows)], own_sem)
    put.start()
    narrow = (
        lax.broadcasted_iota(jnp.int32, (columns, 128), 1) == lax.broadcasted_iota(jnp.int32, (columns, 128), 0)
    ).astype(bf16)
    tile[0:12, :] = dot(vector[...].astype(bf16), narrow, NN)
    tile[12:16, :] = jnp.zeros((4, 128), f32)

    def widen(small, s):
        move = (
            lax.broadcasted_iota(jnp.int32, (128, D), 1) == lax.broadcasted_iota(jnp.int32, (128, D), 0) + s * columns
        ) & (lax.broadcasted_iota(jnp.int32, (128, D), 0) < columns)
        return dot(small.astype(bf16), move.astype(bf16), NN)

    greet(me)
    put.wait()

    def vec_copy(i, k, peer):
        return pltpu.make_async_remote_copy(
            src_ref=vin.at[i], dst_ref=vtmp.at[k], send_sem=vs_sem.at[k], recv_sem=vr_sem.at[k], device_id=peer
        )

    def vec_at(i):
        return pltpu.make_async_remote_copy(
            src_ref=tile, dst_ref=tiles_in.at[i], send_sem=vs_sem.at[2 + i], recv_sem=vr_sem.at[2 + i],
            device_id=me.at((a + i) % na),
        )

    v_y, v_x, v_core = vec_copy(1, 0, me.y_mate()), vec_copy(2, 1, me.x_mate()), vec_copy(3, 2, me.core_mate())
    for i in range(1, na):
        vec_at(i).start()

    @pl.when(a < nq)
    def _():
        for h in range(FINE):
            @pl.when(a + 1 < na)
            def _():
                chain_up(a, h).start()

            @pl.when(a > 0)
            def _():
                chain_down(a, h).start()

        for h in range(FINE // 2):
            x_copy(a, h, FINE).start()
            y_copy(a, h, FINE).start()

    @pl.when(a >= nq)
    def _():
        x_copy(a, 0, HALVES).start()
        y_copy(a, 0, HALVES).start()
        if relay:
            @pl.when(a > 0)
            def _():
                relay_down(a).start()
        else:
            @pl.loop(1, na)
            def _(d):
                @pl.when(d <= a)
                def _():
                    direct(a - d).start()

    def rest(copy):
        @pl.when(a < nq)
        def _():
            for h in range(FINE // 2, FINE):
                copy(a, h, FINE).start()

        @pl.when(a >= nq)
        def _():
            copy(a, 1, HALVES).start()

    total = widen(tile[...], mine)
    for i in range(1, na):
        vec_at(i).wait()
        total = total + widen(tiles_in[i], me.sid((a - i + na) % na, b, y, c))
    vin[1] = total
    v_y.start()
    rest(y_copy)
    pass_chain(0)
    v_y.wait()
    vin[2] = vin[1] + vtmp[0]
    v_x.start()
    rest(x_copy)
    pass_chain(1)
    v_x.wait()
    vin[3] = vin[2] + vtmp[1]
    v_core.start()
    pass_chain(2)
    v_core.wait()
    vec[...] = vin[3] + vtmp[2]

    @pl.when(a < nq)
    def _():
        for h in range(FINE):
            core(a, b, y, h, FINE).start()

    @pl.when(a >= nq)
    def _():
        for h in range(HALVES):
            core(a, b, y, h, HALVES).start()

    for h in range(3, FINE):
        pass_chain(h)

    @pl.when(a >= nq)
    def _():
        if relay:
            @pl.when(a + 1 < na)
            def _():
                relay_up(a).start()
        else:
            @pl.loop(1, na)
            def _(d):
                @pl.when(a + d < na)
                def _():
                    direct(a + d).start()

    if relay:
        take_at(1)

    @pl.when(a >= nq + 1)
    def _():
        pass_plane(a, HALVES)

    for a_ in range(nq):
        pass_plane(a_, FINE)

    if relay:
        first = 1 + (a == 1).astype(jnp.int32)
        second = 2 + ((a == 1) | (a == 2)).astype(jnp.int32)

        @pl.when(a == 0)
        def _():
            share(first)

    loads[2].wait()

    @pl.loop(0, SEQ // 256)
    def _(t):
        at = pl.ds(pl.multiple_of(t * 256, 256), 256)
        x = tokens[at, :]
        centred = x - jnp.mean(x, -1, keepdims=True)
        inverse = lax.rsqrt(jnp.mean(centred * centred, -1, keepdims=True) + EPS)
        n1[at, :] = (centred * inverse * vec[0:1, :] + vec[1:2, :]).astype(bf16)

    @pl.when(a == nq)
    def _():
        pass_plane(a, HALVES)

    if relay:
        take_at(-1)
    for a_ in range(nq):
        pass_diag(a_, FINE)
    if relay:
        take_at(2)
    for a_ in range(nq):
        partner(a_, FINE)
    fetch_q = pltpu.make_async_copy(whole.at[pl.ds(0, 3 * D)], wq, wq_sem)
    fetch_q.start()
    if relay:
        take_at(-2)

        @pl.when(a > 0)
        def _():
            share(first)

    def save(k, src, dst):
        return pltpu.make_async_copy(src, dst, save_sem.at[k])

    save(0, n1, n1_out).start()
    fetch_q.wait()

    def project(begin, row, scale):
        @pl.loop(begin, begin + 3)
        def _(j):
            at = pl.ds(pl.multiple_of(j * 256, 256), 256)
            r = dot(n1[...], wq[at, :], NT)
            if row is not None:
                cols = pl.ds(pl.multiple_of((j - begin) * 256, 256), 256)
                r = r + vec[row:row + 1, cols]
            r = r.astype(bf16)
            if scale is not None:
                r = r * jnp.asarray(scale, bf16)
            qkv[:, at] = r

    project(0, 2, 0.125)
    project(3, None, None)
    project(6, 3, None)
    save(1, qkv, qkv_out).start()

    lo = lax.broadcasted_iota(jnp.int32, (1, 128), 1) < 64
    zero = jnp.zeros((), bf16)

    def attend(i):
        q_at = pl.ds(pl.multiple_of(i * 128, 128), 128)
        k_at = pl.ds(pl.multiple_of(D + i * 128, 128), 128)
        v_at = pl.ds(pl.multiple_of(2 * D + i * 128, 128), 128)
        for qb in range(SEQ // QB):
            span = (qb + 1) * QB
            outs, sums = [], []
            for h in range(2):
                block = qkv[qb * QB:span, q_at]
                block = jnp.where(lo, block, zero) if h == 0 else jnp.where(lo, zero, block)
                s = dot(block, qkv[:span, k_at], NT)
                qi = lax.broadcasted_iota(jnp.int32, (QB, QB), 0)
                ki = lax.broadcasted_iota(jnp.int32, (QB, QB), 1)
                diag = jnp.where(ki <= qi, s[:, span - QB:], NEG)
                s = jnp.concatenate([s[:, :span - QB], diag], 1) if qb else diag
                m = jnp.max(s, 1, keepdims=True)
                p = jnp.exp(s - m)
                l = jnp.sum(p, 1, keepdims=True)
                outs.append(dot(p.astype(bf16), qkv[:span, v_at], NN) / l)
                sums.append(m + jnp.log(l))
            mixed[qb * QB:span, q_at] = jnp.where(lo, outs[0], outs[1]).astype(bf16)
            lc[qb * QB:span, :] = jnp.where(lo, sums[0], sums[1])
        t = jnp.transpose(lc[...], (1, 0))
        lse[i, 0:1, :] = t[0:1]
        lse[i, 1:2, :] = t[64:65]

    def own_diag():
        @pl.when(a >= nq)
        def _():
            pass_diag(a, HALVES)

    def third(act):
        @pl.when(a == 0)
        def _():
            act(3)

    def third_column(a_):
        take(a_)
        share(a_)

    steps = ()
    if relay:
        steps = (
            (0, own_diag),
            (1, lambda: pass_plane(first, HALVES)), (1, lambda: share(second)),
            (3, lambda: pass_diag(first, HALVES)), (3, lambda: third(third_column)),
            (4, lambda: pass_plane(second, HALVES)),
            (5, lambda: pass_diag(second, HALVES)),
        )

    @pl.loop(0, PAIRS)
    def _(i):
        attend(i)
        for k, act_now in steps:
            @pl.when(i == k)
            def _():
                act_now()

    save(2, mixed, mixed_out).start()
    if relay:
        partner(first, HALVES)

        @pl.when(a == 0)
        def _():
            partner(second, HALVES)

        @pl.when(a > 0)
        def _():
            partner(a, HALVES)
    else:
        own_diag()
        for k in range(1, na):
            for a_ in (a + k, a - k):
                @pl.when((a_ >= nq) & (a_ < na))
                def _():
                    take(a_)
                    share(a_)
                    pass_plane(a_, HALVES)
                    pass_diag(a_, HALVES)

        @pl.loop(nq, na)
        def _(a_):
            partner(a_, HALVES)

    def settle():
        if relay:
            third(lambda a_: pass_diag(a_, HALVES))
            third(lambda a_: partner(a_, HALVES))

            @pl.when(a > 0)
            def _():
                partner(second, HALVES)

    fetch_o = pltpu.make_async_copy(whole.at[pl.ds(3 * D, D)], w_out, wq_sem)
    fetch_o.start()
    BLOCKS = FF // 256
    shift = (a == na - 1).astype(jnp.int32) * 3 if relay else 0

    def weights_in(j):
        at = (j + shift) % BLOCKS * 256
        slot = j % 2
        return (
            pltpu.make_async_copy(whole.at[pl.ds(pl.multiple_of(4 * D + at, 256), 256)], wf.at[slot], w_sem.at[slot]),
            pltpu.make_async_copy(
                whole.at[pl.ds(pl.multiple_of(4 * D + FF + at, 256), 256)], wd.at[slot], w_sem.at[2 + slot]
            ),
        )

    for one in weights_in(0):
        one.start()
    loads[3].wait()
    fetch_o.wait()
    length = lengths[0]

    def alive(t):
        return lax.broadcasted_iota(jnp.int32, (256, 1), 0) + t * 256 < length

    @pl.loop(0, SEQ // 256)
    def _(t):
        at = pl.ds(pl.multiple_of(t * 256, 256), 256)
        x = tokens[at, :] + dot(mixed[at, :], w_out[...], NT) + vec[4:5, :]
        after[at, :] = x
        centred = x - jnp.mean(x, -1, keepdims=True)
        inverse = lax.rsqrt(jnp.mean(centred * centred, -1, keepdims=True) + EPS)
        n2[at, :] = (centred * inverse * vec[5:6, :] + vec[6:7, :]).astype(bf16)
        acc[at, :] = x + vec[7:8, :]
        top_low[at, :] = jnp.where(alive(t), cot[at, :], 0.0).astype(bf16)
        ngrad[at, :] = jnp.zeros((256, D), f32)

    if relay:
        third(lambda a_: pass_plane(a_, HALVES))

    def put_grad(k, slot, row):
        return pltpu.make_async_copy(
            stage.at[slot, k], ge.at[pl.ds(pl.multiple_of(row, 256), 256)], stage_sem.at[slot, k]
        )

    def put_both(j):
        at = (j + shift) % BLOCKS * 256
        return put_grad(0, j % 2, D + at), put_grad(1, j % 2, D + FF + at)

    @pl.loop(0, BLOCKS)
    def _(j):
        @pl.when(j == 2)
        def _():
            settle()

        @pl.when(j + 1 < BLOCKS)
        def _():
            for one in weights_in(j + 1):
                one.start()

        for one in weights_in(j):
            one.wait()
        slot = j % 2
        unit = (j + shift) % BLOCKS
        line, cols = 8 + unit // 3, pl.ds(pl.multiple_of(unit % 3 * 256, 256), 256)
        bias = vec[pl.ds(line, 1), cols]
        sums = jnp.zeros((1, 256), f32)
        for t in range(SEQ // 256):
            at = pl.ds(t * 256, 256)
            x = dot(n2[at, :], wf[slot], NT) + bias
            g = dot(top_low[at, :], wd[slot], NT)
            square = x * x
            part = 0.5 + 0.5 * jnp.tanh(ROOT * x * (1.0 + CUBIC * square))
            active = (x * part).astype(bf16)
            slope = part * (1.0 + (2.0 * ROOT) * x * (1.0 - part) * (1.0 + (3.0 * CUBIC) * square))
            g = g * slope
            sums = sums + jnp.sum(g, 0, keepdims=True)
            g = g.astype(bf16)
            act[at, :] = active
            hid[at, :] = g
            acc[at, :] += dot(active, wd[slot], NN)
            ngrad[at, :] += dot(g, wf[slot], NN)
        part_sums[pl.ds(line, 1), cols] = sums

        @pl.when(j >= 2)
        def _():
            for one in put_both(j - 2):
                one.wait()

        stage[slot, 0] = dot(hid[...], n2[...], TN).astype(bf16)
        stage[slot, 1] = dot(act[...], top_low[...], TN).astype(bf16)
        for one in put_both(j):
            one.start()

    part_sums[0:8, :] = jnp.zeros((8, D), f32)
    part_sums[12:16, :] = jnp.zeros((4, D), f32)

    @pl.loop(0, SEQ // 256)
    def _(t):
        at = pl.ds(pl.multiple_of(t * 256, 256), 256)
        live = alive(t)
        x = after[at, :]
        centred = x - jnp.mean(x, -1, keepdims=True)
        inverse = lax.rsqrt(jnp.mean(centred * centred, -1, keepdims=True) + EPS)
        unit = centred * inverse
        g = ngrad[at, :]
        e = g * vec[5:6, :]
        top = jnp.where(live, cot[at, :], 0.0)
        mid = top + inverse * (e - jnp.mean(e, -1, keepdims=True) - unit * jnp.mean(e * unit, -1, keepdims=True))
        low[at, :] = mid.astype(bf16)
        part_sums[4:5, :] += jnp.sum(mid, 0, keepdims=True)
        part_sums[5:6, :] += jnp.sum(g * unit, 0, keepdims=True)
        part_sums[6:7, :] += jnp.sum(g, 0, keepdims=True)
        part_sums[7:8, :] += jnp.sum(top, 0, keepdims=True)
        ngrad[at, :] = mid + jnp.where(live, 0.0, cot[at, :])
        acc[at, :] = jnp.where(live, acc[at, :], tokens[at, :])

    finals = [save(3, low, low_out), save(4, ngrad, base_out), save(5, acc, block_out)]
    for one in finals:
        one.start()
    for j in (BLOCKS - 2, BLOCKS - 1):
        for one in put_both(j):
            one.wait()

    @pl.loop(0, 3)
    def _(j):
        @pl.when(j >= 2)
        def _():
            put_grad(0, 0, 0).wait()

        stage[j % 2, 0] = dot(low[:, pl.ds(pl.multiple_of(j * 256, 256), 256)], mixed[...], TN).astype(bf16)
        put_grad(0, j % 2, j * 256).start()

    put_grad(0, 1, 256).wait()
    put_grad(0, 0, 512).wait()
    for one in [save(0, n1, n1_out), save(1, qkv, qkv_out), save(2, mixed, mixed_out)] + finals:
        one.wait()

    def sent(a_, n):
        for h in range(n):
            x_copy(a_, h, n).wait_send()
            y_copy(a_, h, n).wait_send()
            diag_send(a_, h, n).wait_send()
            for b_, y_ in around:
                core(a_, b_, y_, h, n).wait_send()

    for a_ in range(nq):
        sent(a_, FINE)
        for h in range(FINE):
            @pl.when((a_ <= a) & (a + 1 < na))
            def _():
                chain_up(a_, h).wait_send()

            @pl.when((a_ >= a) & (a > 0))
            def _():
                chain_down(a_, h).wait_send()

    @pl.loop(nq, na)
    def _(a_):
        sent(a_, HALVES)

    if relay:
        @pl.loop(nq, na)
        def _(a_):
            @pl.when((a_ <= a) & (a + 1 < na))
            def _():
                relay_up(a_).wait_send()

            @pl.when((a_ >= a) & (a > 0))
            def _():
                relay_down(a_).wait_send()
    else:
        @pl.when(a >= nq)
        def _():
            @pl.loop(0, na)
            def _(to):
                @pl.when(to != a)
                def _():
                    direct(to).wait_send()


def forward(n_dp, lengths, tokens, master, vector, cotangent):
    na = n_dp // 2
    rows = master.shape[0]
    count = na * 8
    dma = pltpu.SemaphoreType.DMA
    vm, hbm = pl.BlockSpec(memory_space=pltpu.VMEM), pl.BlockSpec(memory_space=pl.ANY)
    wide, full = pltpu.VMEM((SEQ, D), f32), pltpu.VMEM((SEQ, D), bf16)
    block = pltpu.VMEM((2, 256, D), bf16)

    def out(rows, dtype, columns=D):
        return jax.ShapeDtypeStruct((rows, columns), dtype)

    return pl.pallas_call(
        functools.partial(forward_kernel, n_dp),
        in_specs=[pl.BlockSpec(memory_space=pltpu.SMEM), hbm, hbm, hbm, hbm],
        out_specs=[hbm] * 8 + [vm, vm, vm],
        out_shape=[
            out(count * rows, bf16), out(count * rows - 3 * D, bf16), out(SEQ, bf16), out(SEQ, bf16, 3 * D),
            out(SEQ, bf16), out(SEQ, bf16), out(SEQ, f32), out(SEQ, f32), out(16, f32),
            jax.ShapeDtypeStruct((PAIRS, 8, SEQ), f32), out(16, f32),
        ],
        scratch_shapes=[
            wide, pltpu.VMEM((rows, D), f32), pltpu.VMEM(vector.shape, f32), wide, dma((4,)), dma((6,)),
            full, pltpu.VMEM((SEQ, 3 * D), bf16), full, full, wide, wide, wide, full, full,
            pltpu.VMEM((SEQ, 256), bf16), pltpu.VMEM((SEQ, 256), bf16), pltpu.VMEM((D, D), bf16),
            block, block, dma((4,)), pltpu.VMEM((2, 2, 256, D), bf16), dma((2, 2)),
            pltpu.VMEM((rows, D), bf16), dma,
            pltpu.VMEM((3 * D, D), bf16), dma,
            pltpu.VMEM((16, 128), f32), pltpu.VMEM((na, 16, 128), f32),
            pltpu.VMEM((4, 16, D), f32), pltpu.VMEM((3, 16, D), f32), dma((3 + na,)), dma((3 + na,)),
            pltpu.VMEM((SEQ, 128), f32),
            dma((2 * na, FINE)), dma((na, FINE)), dma((na,)), dma((na,)), dma((na,)),
            dma((na, FINE)), dma((na, FINE)),
            dma((na, FINE)), dma((na, FINE)),
            dma((na, FINE)), dma((na, FINE)),
            dma((na, 4, FINE)), dma((na, 4, FINE)),
        ],
        compiler_params=pltpu.CompilerParams(
            collective_id=1, has_side_effects=True, vmem_limit_bytes=66_000_000
        ),
        name="gather_forward",
    )(lengths, tokens, master, vector, cotangent)


def tiles(rows, parts):
    marks = [16 * round(rows * h / parts / 16) for h in range(parts)] + [rows]
    return [(marks[h], marks[h + 1] - marks[h]) for h in range(parts)]


def backward_kernel(
    n_dp, weights, ge, qkv_in, mixed_in, lse, n1_in, low_in, tokens_in, base_in, vec, part,
    gl, out, total, vector_total,
    w_out, w_qkv, qkv, mixed, n1, low, tokens, base, load_sem,
    do, proj, stage, stage_sem, kT, dqT, dk_s, dv_s, dl,
    gbuf, kbuf, dbuf, xbuf, ybuf, zbuf, cbuf, vin, vtmp,
    ls, ks, kr, ds, dr, xs, xr, ys, yr, zs, zr, cs, cr, vs, vr,
):
    me = Place(n_dp)
    na = me.na
    nq = na // 4
    a, b, y, c = me.a, me.b, me.y, me.c
    rows = total.shape[0]
    around = ((b, y), (1 - b, y), (b, 1 - y), (1 - b, 1 - y))
    quarters = tiles(rows, 4)
    early = 3 * D

    def span(q):
        return quarters[2 * q][0], quarters[2 * q][1] + quarters[2 * q + 1][1]

    def grads(a_, o, core, q):
        first, size = span(q)
        at = me.sid(a_, *around[o], core) * rows + first
        if isinstance(a_, int):
            return gl.at[pl.ds(pl.multiple_of(at, 8), size)]
        return ge.at[pl.ds(pl.multiple_of(at - early, 8), size)]

    def fetch(a_, o, q):
        return pltpu.make_async_copy(grads(a_, o, c, q), gbuf.at[a_, o, pl.ds(*span(q))], ls.at[a_, o, q])

    def to_core(a_, o, q):
        return pltpu.make_async_remote_copy(
            src_ref=grads(a_, o, 1 - c, q), dst_ref=kbuf.at[a_, o, pl.ds(*span(q))],
            send_sem=ks.at[a_, o, q], recv_sem=kr.at[a_, o, q], device_id=me.core_mate(),
        )

    def move(src, dst, send, recv, peer):
        return pltpu.make_async_remote_copy(src_ref=src, dst_ref=dst, send_sem=send, recv_sem=recv, device_id=peer)

    def diag(a_, h):
        at = pl.ds(*quarters[h])
        peer = me.x_mate() if h % 2 == 0 else me.y_mate()
        return move(kbuf.at[a_, 3, at], dbuf.at[a_, at], ds.at[a_, h], dr.at[a_, h], peer)

    def x_copy(a_, h):
        at = pl.ds(*quarters[h])
        return move(kbuf.at[a_, 1, at], xbuf.at[a_, at], xs.at[a_, h], xr.at[a_, h], me.x_mate())

    def y_copy(a_, h):
        at = pl.ds(*quarters[h])
        return move(kbuf.at[a_, 2, at], ybuf.at[a_, at], ys.at[a_, h], yr.at[a_, h], me.y_mate())

    def direct(a_, q):
        at = pl.ds(*span(q))
        return move(kbuf.at[a_, 0, at], zbuf.at[a, at], zs.at[a_, q], zr.at[a, q], me.at(a_))

    def direct_from(a_, q):
        at = pl.ds(*span(q))
        return move(kbuf.at[a_, 0, at], zbuf.at[a_, at], zs.at[a_, q], zr.at[a_, q], me.at(a_))

    def chain(a_, h, down):
        at = pl.ds(*quarters[h])
        way = 0 if down else 1
        return move(
            kbuf.at[a_, 0, at], cbuf.at[a_, way, at], cs.at[a_, h], cr.at[a_, way, h], me.at(a - 1 if down else a + 1)
        )

    def add(to, frm):
        kbuf[to] = (kbuf[to].astype(f32) + frm.astype(f32)).astype(bf16)

    def start(a_, q):
        for o in range(4):
            to_core(a_, o, q).start()
            fetch(a_, o, q).start()

    def pair_sum(a_, q):
        at = pl.ds(*span(q))
        for o in (3, 1, 2, 0):
            to_core(a_, o, q).wait_recv()
            fetch(a_, o, q).wait()
            add((a_, o, at), gbuf[a_, o, at])
            if o == 3:
                diag(a_, 2 * q).start()
                diag(a_, 2 * q + 1).start()
            if o == 1:
                x_copy(a_, 2 * q).start()
            if o == 2:
                y_copy(a_, 2 * q + 1).start()

    def diag_sum(a_, q):
        at = pl.ds(*quarters[2 * q])
        diag(a_, 2 * q).wait_recv()
        add((a_, 2, at), dbuf[a_, at])
        y_copy(a_, 2 * q).start()
        at = pl.ds(*quarters[2 * q + 1])
        diag(a_, 2 * q + 1).wait_recv()
        add((a_, 1, at), dbuf[a_, at])
        x_copy(a_, 2 * q + 1).start()

    def plane_sum(a_, h):
        at = pl.ds(*quarters[h])
        x_copy(a_, h).wait_recv()
        y_copy(a_, h).wait_recv()
        add((a_, 0, at), xbuf[a_, at].astype(f32) + ybuf[a_, at].astype(f32))

    def spread(a_, q):
        plane_sum(a_, 2 * q)
        plane_sum(a_, 2 * q + 1)

        @pl.when(a_ != a)
        def _():
            direct(a_, q).start()

    def link(a_, h):
        at = pl.ds(*quarters[h])
        plane_sum(a_, h)

        @pl.when(a > a_)
        def _():
            @pl.when(a + 1 < na)
            def _():
                chain(a_, h, True).wait_recv()
                add((a_, 0, at), cbuf[a_, 0, at])

            chain(a_, h, True).start()

        @pl.when(a < a_)
        def _():
            @pl.when(a > 0)
            def _():
                chain(a_, h, False).wait_recv()
                add((a_, 0, at), cbuf[a_, 1, at])

            chain(a_, h, False).start()

    def item(i):
        return nq + i // 2 + 0 * a, i % 2

    def local(k, src, dst):
        return pltpu.make_async_copy(src, dst, load_sem.at[k])

    loads = [
        local(0, low_in, low), local(1, weights.at[pl.ds(3 * D, D)], w_out), local(2, qkv_in, qkv),
        local(3, mixed_in, mixed), local(4, n1_in, n1), local(5, weights.at[pl.ds(0, 3 * D)], w_qkv),
        local(6, tokens_in, tokens), local(7, base_in, base),
    ]
    for load in loads[:4]:
        load.start()
    greet(me)

    @pl.loop(nq, na)
    def _(a_):
        for q in range(2):
            start(a_, q)

    for load in loads[4:]:
        load.start()
    loads[0].wait()
    loads[1].wait()

    @pl.loop(0, 3)
    def _(j):
        at = pl.ds(pl.multiple_of(j * 256, 256), 256)
        do[:, at] = dot(low[...], w_out[:, at], NN).astype(bf16)

    pair_sum(*item(0))
    pair_sum(*item(1))
    loads[2].wait()
    loads[3].wait()

    lo = lax.broadcasted_iota(jnp.int32, (1, 128), 1) < 64
    zero = jnp.zeros((), bf16)

    def attend_back(i):
        q_at = pl.ds(pl.multiple_of(i * 128, 128), 128)
        k_at = pl.ds(pl.multiple_of(D + i * 128, 128), 128)
        v_at = pl.ds(pl.multiple_of(2 * D + i * 128, 128), 128)
        prod = do[:, q_at].astype(f32) * mixed[:, q_at].astype(f32)
        d0 = jnp.sum(jnp.where(lo, prod, 0.0), 1, keepdims=True)
        d1 = jnp.sum(jnp.where(lo, 0.0, prod), 1, keepdims=True)
        dl[...] = jnp.transpose(jnp.where(lo, d0, d1), (1, 0))
        kT[...] = jnp.transpose(qkv[:, k_at], (1, 0))
        for qb in range(SEQ // QB):
            q0 = qb * QB
            end = q0 + QB
            for h in range(2):
                offset = lse[i, h:h + 1, q0:end]
                delta = dl[64 * h:64 * h + 1, q0:end]
                qm, dm = qkv[q0:end, q_at], do[q0:end, q_at]
                qm = jnp.where(lo, qm, zero) if h == 0 else jnp.where(lo, zero, qm)
                dm = jnp.where(lo, dm, zero) if h == 0 else jnp.where(lo, zero, dm)
                s = dot(qkv[:end, k_at], qm, NT)
                ki = lax.broadcasted_iota(jnp.int32, (QB, QB), 0)
                qi = lax.broadcasted_iota(jnp.int32, (QB, QB), 1)
                last = jnp.where(ki <= qi, s[q0:], NEG)
                s = jnp.concatenate([s[:q0], last], 0) if qb else last
                p = jnp.exp(s - offset)
                dp = dot(qkv[:end, v_at], dm, NT)
                dsc = (p * (dp - delta)).astype(bf16)
                pv = dot(p.astype(bf16), dm, NN)
                pk = dot(dsc, qm, NN)
                if h == 0:
                    if qb:
                        dv_s[:q0, :] += pv[:q0]
                        dk_s[:q0, :] += pk[:q0]
                    dv_s[q0:end, :] = pv[q0:]
                    dk_s[q0:end, :] = pk[q0:]
                else:
                    dv_s[:end, :] += pv
                    dk_s[:end, :] += pk
                dqT[64 * h:64 * h + 64, q0:end] = dot(kT[64 * h:64 * h + 64, :end], dsc, NN)
        dq = jnp.transpose(dqT[...], (1, 0)) * 0.125
        dv = dv_s[...]
        proj[:, q_at] = dq.astype(bf16)
        proj[:, k_at] = dk_s[...].astype(bf16)
        proj[:, v_at] = dv.astype(bf16)
        vin[0, 2:3, q_at] = jnp.sum(dq, 0, keepdims=True)
        vin[0, 3:4, q_at] = jnp.sum(dv, 0, keepdims=True)

    vin[0] = part[...]
    steps = ((0, diag_sum, 0), (1, pair_sum, 2), (1, diag_sum, 1), (2, spread, 0), (2, pair_sum, 3),
             (3, diag_sum, 2), (3, spread, 1), (4, diag_sum, 3), (5, spread, 2), (5, pair_sum, 4))

    @pl.loop(0, PAIRS)
    def _(i):
        attend_back(i)
        for k, act, which in steps:
            @pl.when(i == k)
            def _():
                act(*item(which))

    loads[4].wait()

    def save(j):
        return pltpu.make_async_copy(
            stage.at[j % 2], gl.at[pl.ds(pl.multiple_of(j * 256, 256), 256)], stage_sem.at[j % 2]
        )

    @pl.loop(0, 9)
    def _(j):
        @pl.when(j >= 2)
        def _():
            save(j - 2).wait()

        stage[j % 2] = dot(proj[:, pl.ds(pl.multiple_of(j * 256, 256), 256)], n1[...], TN).astype(bf16)
        save(j).start()

    save(7).wait()
    save(8).wait()
    for a_ in range(nq):
        for q in range(2):
            start(a_, q)
    for load in loads[5:]:
        load.wait()

    def norm_back(t):
        at = pl.ds(t * 256, 256)
        x = tokens[at, :]
        centred = x - jnp.mean(x, -1, keepdims=True)
        inverse = lax.rsqrt(jnp.mean(centred * centred, -1, keepdims=True) + EPS)
        unit = centred * inverse
        g = dot(proj[at, :], w_qkv[...], NN)
        e = g * vec[0:1, :]
        out[at, :] = base[at, :] + inverse * (
            e - jnp.mean(e, -1, keepdims=True) - unit * jnp.mean(e * unit, -1, keepdims=True)
        )
        vin[0, 0:1, :] += jnp.sum(g * unit, 0, keepdims=True)
        vin[0, 1:2, :] += jnp.sum(g, 0, keepdims=True)

    def after(t):
        if t == 0:
            for a_ in range(nq):
                for q in range(2):
                    pair_sum(a_, q)
        if t == 1:
            diag_sum(*item(4))
            spread(*item(3))
        if t == 2:
            for a_ in range(nq):
                diag_sum(a_, 0)
                diag_sum(a_, 1)
            pair_sum(*item(5))
        if t == 3:
            spread(*item(4))

    for t in range(4):
        norm_back(t)
        after(t)

    def vec_copy(i, k, peer):
        return pltpu.make_async_remote_copy(
            src_ref=vin.at[i], dst_ref=vtmp.at[k], send_sem=vs.at[k], recv_sem=vr.at[k], device_id=peer
        )

    v_core, v_y, v_x = vec_copy(0, 0, me.core_mate()), vec_copy(1, 1, me.y_mate()), vec_copy(2, 2, me.x_mate())

    def vec_at(i):
        return vec_copy(3, 2 + i, me.at((a + i) % na))

    v_core.start()
    diag_sum(*item(5))
    v_core.wait()
    vin[1] = vin[0] + vtmp[0]
    v_y.start()
    for a_ in range(nq):
        link(a_, 0)
        link(a_, 1)
    v_y.wait()
    vin[2] = vin[1] + vtmp[1]
    v_x.start()
    for a_ in range(nq):
        link(a_, 2)
        link(a_, 3)
    v_x.wait()
    vin[3] = vin[2] + vtmp[2]
    for i in range(1, na):
        vec_at(i).start()
    spread(*item(5))

    if na > 4:
        @pl.loop(nq + 3, na)
        def _(a_):
            for q in range(2):
                pair_sum(a_, q)
                diag_sum(a_, q)
                spread(a_, q)

    vsum = vin[3]
    for i in range(1, na):
        vec_at(i).wait()
        vsum = vsum + vtmp[2 + i]
    vector_total[...] = vsum

    @pl.when(a >= nq)
    def _():
        total[...] = kbuf[a, 0].astype(f32)

        @pl.loop(1, na)
        def _(i):
            frm = (a + i) % na
            for q in range(2):
                direct_from(frm, q).wait_recv()
            total[...] += zbuf[frm].astype(f32)

    for a_ in range(nq):
        @pl.when(a == a_)
        def _():
            total[...] = kbuf[a_, 0].astype(f32)

            @pl.when(a + 1 < na)
            def _():
                for h in range(4):
                    chain(a_, h, True).wait_recv()
                total[...] += cbuf[a_, 0].astype(f32)

            @pl.when(a > 0)
            def _():
                for h in range(4):
                    chain(a_, h, False).wait_recv()
                total[...] += cbuf[a_, 1].astype(f32)

        @pl.when(a != a_)
        def _():
            for h in range(4):
                chain(a_, h, True).wait_send()

    def sent(a_):
        for q in range(2):
            for o in range(4):
                to_core(a_, o, q).wait_send()
        for h in range(4):
            diag(a_, h).wait_send()
            x_copy(a_, h).wait_send()
            y_copy(a_, h).wait_send()

    for a_ in range(nq):
        sent(a_)

    @pl.loop(nq, na)
    def _(a_):
        sent(a_)

        @pl.when(a_ != a)
        def _():
            for q in range(2):
                direct(a_, q).wait_send()


def backward(n_dp, rows, weights, ge, qkv, mixed, lse, n1, low, tokens, base, vec, part):
    na = n_dp // 2
    nq = na // 4
    dma = pltpu.SemaphoreType.DMA
    vm, anyw = pl.BlockSpec(memory_space=pltpu.VMEM), pl.BlockSpec(memory_space=pl.ANY)
    full = pltpu.VMEM((SEQ, D), bf16)
    wide = pltpu.VMEM((SEQ, D), f32)
    return pl.pallas_call(
        functools.partial(backward_kernel, n_dp),
        in_specs=[anyw, anyw, anyw, anyw, vm, anyw, anyw, anyw, anyw, vm, vm],
        out_specs=[anyw, vm, vm, vm],
        out_shape=[
            jax.ShapeDtypeStruct((3 * D, D), bf16),
            jax.ShapeDtypeStruct((SEQ, D), f32),
            jax.ShapeDtypeStruct((rows, D), f32),
            jax.ShapeDtypeStruct((16, D), f32),
        ],
        scratch_shapes=[
            pltpu.VMEM((D, D), bf16), pltpu.VMEM((3 * D, D), bf16), pltpu.VMEM((SEQ, 3 * D), bf16),
            full, full, full, wide, wide, dma((8,)),
            full, pltpu.VMEM((SEQ, 3 * D), bf16), pltpu.VMEM((2, 256, D), bf16), dma((2,)),
            pltpu.VMEM((128, SEQ), bf16), pltpu.VMEM((128, SEQ), f32),
            pltpu.VMEM((SEQ, 128), f32), pltpu.VMEM((SEQ, 128), f32), pltpu.VMEM((128, SEQ), f32),
            pltpu.VMEM((na, 4, rows, D), bf16), pltpu.VMEM((na, 4, rows, D), bf16),
            pltpu.VMEM((na, rows, D), bf16), pltpu.VMEM((na, rows, D), bf16),
            pltpu.VMEM((na, rows, D), bf16), pltpu.VMEM((na, rows, D), bf16),
            pltpu.VMEM((nq, 2, rows, D), bf16),
            pltpu.VMEM((4, 16, D), f32), pltpu.VMEM((2 + na, 16, D), f32),
            dma((na, 4, 2)), dma((na, 4, 2)), dma((na, 4, 2)),
            dma((na, 4)), dma((na, 4)), dma((na, 4)), dma((na, 4)), dma((na, 4)), dma((na, 4)),
            dma((na, 2)), dma((na, 2)), dma((nq, 4)), dma((nq, 2, 4)), dma((2 + na,)), dma((2 + na,)),
        ],
        compiler_params=pltpu.CompilerParams(
            collective_id=2, has_side_effects=True, vmem_limit_bytes=66_000_000
        ),
        name="attend_reduce",
    )(weights, ge, qkv, mixed, lse, n1, low, tokens, base, vec, part)


BETA_ONE = 0.9
BETA_TWO = 0.95
ADAM_EPS = 1e-08
ADAM_STEP = 2
LR_MATRIX = 0.05
LR_VECTOR = 0.1
DECAY = 0.1
GRAD_FACTOR = 4.0


def adamw(master, gradient, moment, square, rate, decay):
    moment_new = BETA_ONE * moment + (1.0 - BETA_ONE) * gradient
    square_new = BETA_TWO * square + (1.0 - BETA_TWO) * gradient * gradient
    first_fix = 1.0 - BETA_ONE**ADAM_STEP
    second_fix = 1.0 - BETA_TWO**ADAM_STEP
    stride = moment_new / first_fix / (jnp.sqrt(square_new / second_fix) + ADAM_EPS)
    return (master - rate * (stride + decay * master), moment_new, square_new)


def body(
    tokens, cotangent, lengths, master_matrix, master_vector,
    moment_matrix, moment_vector, square_matrix, square_vector,
):
    n_dp, n_zero = lax.axis_size("dp"), lax.axis_size("zero")
    weights, early, normed_one, qkv, mixed, mid_low, base, block_out, vectors, lse, part = forward(
        n_dp, lengths, tokens, master_matrix, master_vector, cotangent
    )
    late, input_gradient, matrix_total, vector_sum = backward(
        n_dp, master_matrix.shape[0], weights, early, qkv, mixed, lse, normed_one, mid_low, tokens, base, vectors, part
    )
    columns = master_vector.shape[1]
    mine = (lax.axis_index("dp") * n_zero + lax.axis_index("zero")) * columns
    vector_total = lax.dynamic_slice(vector_sum, (0, mine), (12, columns))
    scale = GRAD_FACTOR * float(SEQ * n_dp * n_zero) ** (-0.5)
    matrix_gradient = matrix_total * scale
    vector_gradient = vector_total * scale
    matrix_weights, matrix_moment, matrix_square = adamw(
        master_matrix, matrix_gradient, moment_matrix, square_matrix, LR_MATRIX, DECAY
    )
    vector_weights, vector_moment, vector_square = adamw(
        master_vector, vector_gradient, moment_vector, square_vector, LR_VECTOR, 0.0
    )
    return (
        block_out, input_gradient, matrix_gradient, vector_gradient, matrix_weights,
        vector_weights, matrix_moment, vector_moment, matrix_square, vector_square,
    )


def solution(mesh):
    rows, columns = P(("dp", "zero"), None), P(None, ("dp", "zero"))
    return jax.shard_map(
        body,
        mesh=mesh,
        in_specs=(rows, rows, P(("dp", "zero")), rows, columns, rows, columns, rows, columns),
        out_specs=(rows, rows, rows, columns, rows, columns, rows, columns, rows, columns),
        check_vma=False,
    )
```

```python
import functools
import jax, jax.numpy as jnp
from jax import lax
from jax.experimental import pallas as pl
from jax.experimental.pallas import tpu as pltpu
from jax.sharding import PartitionSpec as P

f32, bf16 = jnp.float32, jnp.bfloat16
D = 768
SEQ = 1024
PAIRS = 6
FF = 3072
EPS = 1e-05
NEG = -1e30
CUBIC = 0.044715
ROOT = 0.7978845608028654
QB = 256
NT = (((1,), (1,)), ((), ()))
NN = (((1,), (0,)), ((), ()))
TN = (((0,), (0,)), ((), ()))


def dot(a, b, dn):
    return lax.dot_general(a, b, dn, preferred_element_type=f32)


def cuts(rows, parts):
    marks = [8 * round(rows * h / parts / 8) for h in range(parts + 1)]
    return [(marks[h], marks[h + 1] - marks[h]) for h in range(parts)]


class Place:
    def __init__(self, n_dp):
        self.na = n_dp // 2
        dp, zero = lax.axis_index("dp"), lax.axis_index("zero")
        self.a, self.b, self.y, self.c = dp // 2, dp % 2, zero // 2, zero % 2

    def sid(self, a, b, y, c):
        return ((a * 2 + b) * 2 + y) * 2 + c

    def dev(self, a, b, y, c):
        return {"dp": a * 2 + b, "zero": y * 2 + c}

    def x_mate(self):
        return self.dev(self.a, 1 - self.b, self.y, self.c)

    def y_mate(self):
        return self.dev(self.a, self.b, 1 - self.y, self.c)

    def core_mate(self):
        return self.dev(self.a, self.b, self.y, 1 - self.c)

    def plane_mate(self, r):
        b = 1 - self.b if r & 1 else self.b
        y = 1 - self.y if r & 2 else self.y
        return self.dev(self.a, b, y, 1 - self.c if r & 4 else self.c)

    def at(self, a):
        return self.dev(a, self.b, self.y, self.c)


def greet(me, peers):
    barrier = pltpu.get_barrier_semaphore()
    for peer in peers:
        pl.semaphore_signal(barrier, inc=1, device_id=peer)
    for i in range(1, me.na):
        pl.semaphore_signal(barrier, inc=1, device_id=me.at((me.a + i) % me.na))
    pl.semaphore_wait(barrier, me.na - 1 + len(peers))


FINE = 4
HALVES = 2


def forward_kernel(
    n_dp, lengths, tokens_in, master_in, vector_in, cot_in,
    whole, ge, n1_out, qkv_out, mixed_out, low_out, base_out, block_out, vec, lse, part_sums,
    tokens, master, vector, cot, load_sem, save_sem,
    n1, qkv, mixed, low, after, acc, ngrad, n2, top_low, act, hid, w_out, wf, wd, w_sem, stage, stage_sem,
    own, own_sem, wq, wq_sem, tile, tiles_in, vin, vtmp, vs_sem, vr_sem, lc,
    ch_s, ch_r, up_s, dn_s, ds, xs, xr, ys, yr, fs, fr, ks, kr,
):
    me = Place(n_dp)
    na = me.na
    nq = na // 4
    a, b, y, c = me.a, me.b, me.y, me.c
    rows = master.shape[0]
    relay = na == 4
    around = ((b, y), (1 - b, y), (b, 1 - y), (1 - b, 1 - y))

    def remote(s, h, n, send, recv, peer):
        first, size = cuts(rows, n)[h]
        ref = whole.at[pl.ds(pl.multiple_of(s * rows + first, 8), size)]
        return pltpu.make_async_remote_copy(
            src_ref=ref, dst_ref=ref, send_sem=send, recv_sem=recv, device_id=peer
        )

    def chain_down(a_, h):
        return remote(me.sid(a_, b, y, c), h, FINE, ch_s.at[a_, h], ch_r.at[a_, h], me.at(a - 1))

    def chain_up(a_, h):
        return remote(me.sid(a_, b, y, c), h, FINE, ch_s.at[na + a_, h], ch_r.at[a_, h], me.at(a + 1))

    def direct(to):
        return remote(me.sid(a, b, y, c), 0, 1, ds.at[to], ch_r.at[a, 0], me.at(to))

    def direct_from(a_):
        return remote(me.sid(a_, b, y, c), 0, 1, ds.at[a_], ch_r.at[a_, 0], me.at(a_))

    def x_copy(a_, h, n, mine=True):
        return remote(me.sid(a_, b if mine else 1 - b, y, c), h, n, xs.at[a_, h], xr.at[a_, h], me.x_mate())

    def y_copy(a_, h, n, mine=True):
        return remote(me.sid(a_, b, y if mine else 1 - y, c), h, n, ys.at[a_, h], yr.at[a_, h], me.y_mate())

    def diag_send(a_, h, n):
        if h < n // 2:
            return remote(me.sid(a_, 1 - b, y, c), h, n, fs.at[a_, h], fr.at[a_, h], me.y_mate())
        return remote(me.sid(a_, b, 1 - y, c), h, n, fs.at[a_, h], fr.at[a_, h], me.x_mate())

    def diag_recv(a_, h, n):
        return remote(me.sid(a_, 1 - b, 1 - y, c), h, n, fs.at[a_, h], fr.at[a_, h], me.x_mate())

    def core(a_, b_, y_, h, n, mine=True):
        o = (b_ + b) % 2 + 2 * ((y_ + y) % 2)
        return remote(
            me.sid(a_, b_, y_, c if mine else 1 - c), h, n, ks.at[a_, o, h], kr.at[a_, o, h], me.core_mate()
        )

    def column_sends(a_, h, n):
        x_copy(a_, h, n).start()
        y_copy(a_, h, n).start()
        core(a_, b, y, h, n).start()

    def pass_chain(h):
        for a_ in range(nq):
            @pl.when(a != a_)
            def _():
                chain_up(a_, h).wait_recv()

                @pl.when((a_ < a) & (a + 1 < na))
                def _():
                    chain_up(a_, h).start()

                @pl.when((a_ > a) & (a > 0))
                def _():
                    chain_down(a_, h).start()

                column_sends(a_, h, FINE)

    def relay_up(a_):
        return remote(me.sid(a_, b, y, c), 0, 1, up_s.at[a_], ch_r.at[a_, 0], me.at(a + 1))

    def relay_down(a_):
        return remote(me.sid(a_, b, y, c), 0, 1, dn_s.at[a_], ch_r.at[a_, 0], me.at(a - 1))

    def take(a_):
        direct_from(a_).wait_recv()
        if relay:
            @pl.when((a_ < a) & (a + 1 < na))
            def _():
                relay_up(a_).start()

            @pl.when((a_ > a) & (a > 0))
            def _():
                relay_down(a_).start()

    def share(a_):
        for h in range(HALVES):
            column_sends(a_, h, HALVES)

    def pass_plane(a_, n):
        for h in range(n):
            x_copy(a_, h, n, False).wait_recv()
            if h < n // 2:
                diag_send(a_, h, n).start()
            core(a_, 1 - b, y, h, n).start()
            y_copy(a_, h, n, False).wait_recv()
            if h >= n // 2:
                diag_send(a_, h, n).start()
            core(a_, b, 1 - y, h, n).start()

    def pass_diag(a_, n):
        for h in range(n):
            diag_recv(a_, h, n).wait_recv()
            core(a_, 1 - b, 1 - y, h, n).start()

    def partner(a_, n):
        for b_, y_ in around:
            for h in range(n):
                core(a_, b_, y_, h, n, False).wait_recv()

    def load(k, src, dst):
        return pltpu.make_async_copy(src, dst, load_sem.at[k])

    loads = [load(0, master_in, master), load(1, vector_in, vector), load(2, tokens_in, tokens), load(3, cot_in, cot)]
    for one in loads:
        one.start()
    mine = me.sid(a, b, y, c)
    columns = vector.shape[1]
    loads[0].wait()
    loads[1].wait()
    own[...] = master[...].astype(bf16)
    put = pltpu.make_async_copy(own, whole.at[pl.ds(pl.multiple_of(mine * rows, 8), rows)], own_sem)
    put.start()
    narrow = (
        lax.broadcasted_iota(jnp.int32, (columns, 128), 1) == lax.broadcasted_iota(jnp.int32, (columns, 128), 0)
    ).astype(bf16)
    tile[0:12, :] = dot(vector[...].astype(bf16), narrow, NN)
    tile[12:16, :] = jnp.zeros((4, 128), f32)

    def widen(small, s):
        move = (
            lax.broadcasted_iota(jnp.int32, (128, D), 1) == lax.broadcasted_iota(jnp.int32, (128, D), 0) + s * columns
        ) & (lax.broadcasted_iota(jnp.int32, (128, D), 0) < columns)
        return dot(small.astype(bf16), move.astype(bf16), NN)

    greet(me, [me.plane_mate(r) for r in range(1, 8)])
    put.wait()

    def vec_copy(r):
        return pltpu.make_async_remote_copy(
            src_ref=vin, dst_ref=vtmp.at[r], send_sem=vs_sem.at[r], recv_sem=vr_sem.at[r],
            device_id=me.plane_mate(r),
        )

    def vec_at(i):
        return pltpu.make_async_remote_copy(
            src_ref=tile, dst_ref=tiles_in.at[i], send_sem=vs_sem.at[7 + i], recv_sem=vr_sem.at[7 + i],
            device_id=me.at((a + i) % na),
        )

    for i in range(1, na):
        vec_at(i).start()

    @pl.when(a < nq)
    def _():
        for h in range(FINE):
            @pl.when(a + 1 < na)
            def _():
                chain_up(a, h).start()

            @pl.when(a > 0)
            def _():
                chain_down(a, h).start()

        for h in range(FINE // 2):
            x_copy(a, h, FINE).start()
            y_copy(a, h, FINE).start()

    @pl.when(a >= nq)
    def _():
        x_copy(a, 0, HALVES).start()
        y_copy(a, 0, HALVES).start()
        if relay:
            @pl.when(a > 0)
            def _():
                relay_down(a).start()
        else:
            @pl.loop(1, na)
            def _(d):
                @pl.when(d <= a)
                def _():
                    direct(a - d).start()

    def rest():
        for copy in (x_copy, y_copy):
            copy(a, 1, HALVES).start()

    total = widen(tile[...], mine)
    for i in range(1, na):
        vec_at(i).wait()
        total = total + widen(tiles_in[i], me.sid((a - i + na) % na, b, y, c))
    vin[...] = total.astype(bf16)
    for r in range(1, 8):
        vec_copy(r).start()

    @pl.when(a < nq)
    def _():
        for h in range(FINE // 2, FINE):
            x_copy(a, h, FINE).start()
            y_copy(a, h, FINE).start()

    @pl.when(a > nq if relay else a >= nq)
    def _():
        rest()

    def at_slot(slot):
        for k in range(na if relay else 0):
            acts = plan[k].get(slot, ())

            if acts:
                @pl.when(a == k)
                def _():
                    for act_now, plane in acts:
                        act_now(plane)

    def plane(a_):
        pass_plane(a_, HALVES)

    def diagonal(a_):
        pass_diag(a_, HALVES)

    def partners(a_):
        partner(a_, HALVES)

    plan = (
        {
            "chain": ((take, 1),), "plane": ((share, 1),), "v": ((take, 2), (share, 2)), 1: ((plane, 1),),
            3: ((diagonal, 1),), 4: ((take, 3), (share, 3)), 5: ((plane, 2),),
            "feed": ((diagonal, 2), (partners, 1), (partners, 2)), "out": ((plane, 3),),
            "all": ((diagonal, 3), (partners, 3)),
        },
        {
            "chain": ((take, 2),), "plane": ((lambda a_: rest(), 1), (share, 2)), "q": ((take, 3),),
            "v": ((plane, 1),), 0: ((share, 3),), 1: ((diagonal, 1),), 2: ((plane, 2),), 4: ((diagonal, 2),),
            5: ((plane, 3),), "feed": ((partners, 1), (partners, 2)), "out": ((diagonal, 3),), "all": ((partners, 3),),
        },
        {
            "middle": ((take, 3),), "chain": ((plane, 2),), "plane": ((share, 3),), "q": ((take, 1), (share, 1)),
            "v": ((diagonal, 2),), 2: ((plane, 3),), 4: ((diagonal, 3),), 5: ((plane, 1),),
            "feed": ((diagonal, 1), (partners, 2), (partners, 1)), "all": ((partners, 3),),
        },
        {
            "middle": ((plane, 3),), "norm": ((take, 2), (share, 2)), "q": ((diagonal, 3),),
            0: ((take, 1), (share, 1)), 2: ((plane, 2),), 4: ((diagonal, 2),), 5: ((plane, 1),),
            "feed": ((diagonal, 1), (partners, 3), (partners, 2), (partners, 1)),
        },
    )
    pass_chain(0)
    vec_total = vin[...].astype(f32)
    for r in range(1, 8):
        vec_copy(r).wait()
        vec_total = vec_total + vtmp[r].astype(f32)
    vec[...] = vec_total

    @pl.when(a < nq)
    def _():
        for h in range(FINE):
            core(a, b, y, h, FINE).start()

    @pl.when(a >= nq)
    def _():
        for h in range(HALVES):
            core(a, b, y, h, HALVES).start()

    for h in range(1, FINE):
        pass_chain(h)
        if h == FINE // 2 - 1:
            at_slot("middle")

    @pl.when(a >= nq)
    def _():
        if relay:
            @pl.when(a + 1 < na)
            def _():
                relay_up(a).start()
        else:
            @pl.loop(1, na)
            def _(d):
                @pl.when(a + d < na)
                def _():
                    direct(a + d).start()

    at_slot("chain")
    if not relay:
        @pl.when(a >= nq + 1)
        def _():
            pass_plane(a, HALVES)

    for a_ in range(nq):
        pass_plane(a_, FINE)
    at_slot("plane")
    loads[2].wait()

    @pl.loop(0, SEQ // 256)
    def _(t):
        at = pl.ds(pl.multiple_of(t * 256, 256), 256)
        x = tokens[at, :]
        centred = x - jnp.mean(x, -1, keepdims=True)
        inverse = lax.rsqrt(jnp.mean(centred * centred, -1, keepdims=True) + EPS)
        n1[at, :] = (centred * inverse * vec[0:1, :] + vec[1:2, :]).astype(bf16)

    if not relay:
        @pl.when(a == nq)
        def _():
            pass_plane(a, HALVES)

    at_slot("norm")
    for a_ in range(nq):
        pass_diag(a_, FINE)
    for a_ in range(nq):
        partner(a_, FINE)
    fetch_q = pltpu.make_async_copy(whole.at[pl.ds(0, 3 * D)], wq, wq_sem)
    fetch_q.start()

    def save(k, src, dst):
        return pltpu.make_async_copy(src, dst, save_sem.at[k])

    save(0, n1, n1_out).start()
    fetch_q.wait()

    def project(begin, row, scale):
        @pl.loop(begin, begin + 3)
        def _(j):
            at = pl.ds(pl.multiple_of(j * 256, 256), 256)
            r = dot(n1[...], wq[at, :], NT)
            if row is not None:
                cols = pl.ds(pl.multiple_of((j - begin) * 256, 256), 256)
                r = r + vec[row:row + 1, cols]
            r = r.astype(bf16)
            if scale is not None:
                r = r * jnp.asarray(scale, bf16)
            qkv[:, at] = r

    project(0, 2, 0.125)
    at_slot("q")
    project(3, None, None)
    project(6, 3, None)
    at_slot("v")
    save(1, qkv, qkv_out).start()

    lo = lax.broadcasted_iota(jnp.int32, (1, 128), 1) < 64
    zero = jnp.zeros((), bf16)

    def attend(i):
        q_at = pl.ds(pl.multiple_of(i * 128, 128), 128)
        k_at = pl.ds(pl.multiple_of(D + i * 128, 128), 128)
        v_at = pl.ds(pl.multiple_of(2 * D + i * 128, 128), 128)
        for qb in range(SEQ // QB):
            span = (qb + 1) * QB
            outs, sums = [], []
            for h in range(2):
                block = qkv[qb * QB:span, q_at]
                block = jnp.where(lo, block, zero) if h == 0 else jnp.where(lo, zero, block)
                s = dot(block, qkv[:span, k_at], NT)
                qi = lax.broadcasted_iota(jnp.int32, (QB, QB), 0)
                ki = lax.broadcasted_iota(jnp.int32, (QB, QB), 1)
                diag = jnp.where(ki <= qi, s[:, span - QB:], NEG)
                s = jnp.concatenate([s[:, :span - QB], diag], 1) if qb else diag
                m = jnp.max(s, 1, keepdims=True)
                p = jnp.exp(s - m)
                l = jnp.sum(p, 1, keepdims=True)
                outs.append(dot(p.astype(bf16), qkv[:span, v_at], NN) / l)
                sums.append(m + jnp.log(l))
            mixed[qb * QB:span, q_at] = jnp.where(lo, outs[0], outs[1]).astype(bf16)
            lc[qb * QB:span, :] = jnp.where(lo, sums[0], sums[1])
        t = jnp.transpose(lc[...], (1, 0))
        lse[i, 0:1, :] = t[0:1]
        lse[i, 1:2, :] = t[64:65]

    @pl.loop(0, PAIRS)
    def _(i):
        attend(i)
        for k in range(PAIRS):
            if relay:
                @pl.when(i == k)
                def _():
                    at_slot(k)

    save(2, mixed, mixed_out).start()
    at_slot("feed")
    if not relay:
        @pl.when(a >= nq)
        def _():
            pass_diag(a, HALVES)

        for k in range(1, na):
            for a_ in (a + k, a - k):
                @pl.when((a_ >= nq) & (a_ < na))
                def _():
                    take(a_)
                    share(a_)
                    pass_plane(a_, HALVES)
                    pass_diag(a_, HALVES)

        @pl.loop(nq, na)
        def _(a_):
            partner(a_, HALVES)

    fetch_o = pltpu.make_async_copy(whole.at[pl.ds(3 * D, D)], w_out, wq_sem)
    fetch_o.start()
    BLOCKS = FF // 256

    def weights_in(j):
        at = j * 256
        slot = j % 2
        return (
            pltpu.make_async_copy(whole.at[pl.ds(pl.multiple_of(4 * D + at, 256), 256)], wf.at[slot], w_sem.at[slot]),
            pltpu.make_async_copy(
                whole.at[pl.ds(pl.multiple_of(4 * D + FF + at, 256), 256)], wd.at[slot], w_sem.at[2 + slot]
            ),
        )

    for one in weights_in(0):
        one.start()
    loads[3].wait()
    fetch_o.wait()
    length = lengths[0]

    def alive(t):
        return lax.broadcasted_iota(jnp.int32, (256, 1), 0) + t * 256 < length

    @pl.loop(0, SEQ // 256)
    def _(t):
        at = pl.ds(pl.multiple_of(t * 256, 256), 256)
        x = tokens[at, :] + dot(mixed[at, :], w_out[...], NT) + vec[4:5, :]
        after[at, :] = x
        centred = x - jnp.mean(x, -1, keepdims=True)
        inverse = lax.rsqrt(jnp.mean(centred * centred, -1, keepdims=True) + EPS)
        n2[at, :] = (centred * inverse * vec[5:6, :] + vec[6:7, :]).astype(bf16)
        acc[at, :] = x + vec[7:8, :]
        top_low[at, :] = jnp.where(alive(t), cot[at, :], 0.0).astype(bf16)
        ngrad[at, :] = jnp.zeros((256, D), f32)

    at_slot("out")

    def put_grad(k, slot, row):
        return pltpu.make_async_copy(
            stage.at[slot, k], ge.at[pl.ds(pl.multiple_of(row, 256), 256)], stage_sem.at[slot, k]
        )

    def put_both(j):
        at = j * 256
        return put_grad(0, j % 2, D + at), put_grad(1, j % 2, D + FF + at)

    @pl.loop(0, BLOCKS)
    def _(j):
        @pl.when(j == 2)
        def _():
            at_slot("all")

        @pl.when(j + 1 < BLOCKS)
        def _():
            for one in weights_in(j + 1):
                one.start()

        for one in weights_in(j):
            one.wait()
        slot = j % 2
        unit = j
        line, cols = 8 + unit // 3, pl.ds(pl.multiple_of(unit % 3 * 256, 256), 256)
        bias = vec[pl.ds(line, 1), cols]
        sums = jnp.zeros((1, 256), f32)
        for t in range(SEQ // 256):
            at = pl.ds(t * 256, 256)
            x = dot(n2[at, :], wf[slot], NT) + bias
            g = dot(top_low[at, :], wd[slot], NT)
            square = x * x
            part = 0.5 + 0.5 * jnp.tanh(ROOT * x * (1.0 + CUBIC * square))
            active = (x * part).astype(bf16)
            slope = part * (1.0 + (2.0 * ROOT) * x * (1.0 - part) * (1.0 + (3.0 * CUBIC) * square))
            g = g * slope
            sums = sums + jnp.sum(g, 0, keepdims=True)
            g = g.astype(bf16)
            act[at, :] = active
            hid[at, :] = g
            acc[at, :] += dot(active, wd[slot], NN)
            ngrad[at, :] += dot(g, wf[slot], NN)
        part_sums[pl.ds(line, 1), cols] = sums

        @pl.when(j >= 2)
        def _():
            for one in put_both(j - 2):
                one.wait()

        stage[slot, 0] = dot(hid[...], n2[...], TN).astype(bf16)
        stage[slot, 1] = dot(act[...], top_low[...], TN).astype(bf16)
        for one in put_both(j):
            one.start()

    part_sums[0:8, :] = jnp.zeros((8, D), f32)
    part_sums[12:16, :] = jnp.zeros((4, D), f32)

    @pl.loop(0, SEQ // 256)
    def _(t):
        at = pl.ds(pl.multiple_of(t * 256, 256), 256)
        live = alive(t)
        x = after[at, :]
        centred = x - jnp.mean(x, -1, keepdims=True)
        inverse = lax.rsqrt(jnp.mean(centred * centred, -1, keepdims=True) + EPS)
        unit = centred * inverse
        g = ngrad[at, :]
        e = g * vec[5:6, :]
        top = jnp.where(live, cot[at, :], 0.0)
        mid = top + inverse * (e - jnp.mean(e, -1, keepdims=True) - unit * jnp.mean(e * unit, -1, keepdims=True))
        low[at, :] = mid.astype(bf16)
        part_sums[4:5, :] += jnp.sum(mid, 0, keepdims=True)
        part_sums[5:6, :] += jnp.sum(g * unit, 0, keepdims=True)
        part_sums[6:7, :] += jnp.sum(g, 0, keepdims=True)
        part_sums[7:8, :] += jnp.sum(top, 0, keepdims=True)
        ngrad[at, :] = mid + jnp.where(live, 0.0, cot[at, :])
        acc[at, :] = jnp.where(live, acc[at, :], tokens[at, :])

    finals = [save(3, low, low_out), save(4, ngrad, base_out), save(5, acc, block_out)]
    for one in finals:
        one.start()
    for j in (BLOCKS - 2, BLOCKS - 1):
        for one in put_both(j):
            one.wait()

    @pl.loop(0, 3)
    def _(j):
        @pl.when(j >= 2)
        def _():
            put_grad(0, 0, 0).wait()

        stage[j % 2, 0] = dot(low[:, pl.ds(pl.multiple_of(j * 256, 256), 256)], mixed[...], TN).astype(bf16)
        put_grad(0, j % 2, j * 256).start()

    put_grad(0, 1, 256).wait()
    put_grad(0, 0, 512).wait()
    for one in [save(0, n1, n1_out), save(1, qkv, qkv_out), save(2, mixed, mixed_out)] + finals:
        one.wait()

    def sent(a_, n):
        for h in range(n):
            x_copy(a_, h, n).wait_send()
            y_copy(a_, h, n).wait_send()
            diag_send(a_, h, n).wait_send()
            for b_, y_ in around:
                core(a_, b_, y_, h, n).wait_send()

    for a_ in range(nq):
        sent(a_, FINE)
        for h in range(FINE):
            @pl.when((a_ <= a) & (a + 1 < na))
            def _():
                chain_up(a_, h).wait_send()

            @pl.when((a_ >= a) & (a > 0))
            def _():
                chain_down(a_, h).wait_send()

    @pl.loop(nq, na)
    def _(a_):
        sent(a_, HALVES)

    if relay:
        @pl.loop(nq, na)
        def _(a_):
            @pl.when((a_ <= a) & (a + 1 < na))
            def _():
                relay_up(a_).wait_send()

            @pl.when((a_ >= a) & (a > 0))
            def _():
                relay_down(a_).wait_send()
    else:
        @pl.when(a >= nq)
        def _():
            @pl.loop(0, na)
            def _(to):
                @pl.when(to != a)
                def _():
                    direct(to).wait_send()


def forward(n_dp, lengths, tokens, master, vector, cotangent):
    na = n_dp // 2
    rows = master.shape[0]
    count = na * 8
    dma = pltpu.SemaphoreType.DMA
    vm, hbm = pl.BlockSpec(memory_space=pltpu.VMEM), pl.BlockSpec(memory_space=pl.ANY)
    wide, full = pltpu.VMEM((SEQ, D), f32), pltpu.VMEM((SEQ, D), bf16)
    block = pltpu.VMEM((2, 256, D), bf16)

    def out(rows, dtype, columns=D):
        return jax.ShapeDtypeStruct((rows, columns), dtype)

    return pl.pallas_call(
        functools.partial(forward_kernel, n_dp),
        in_specs=[pl.BlockSpec(memory_space=pltpu.SMEM), hbm, hbm, hbm, hbm],
        out_specs=[hbm] * 8 + [vm, vm, vm],
        out_shape=[
            out(count * rows, bf16), out(count * rows - 3 * D, bf16), out(SEQ, bf16), out(SEQ, bf16, 3 * D),
            out(SEQ, bf16), out(SEQ, bf16), out(SEQ, f32), out(SEQ, f32), out(16, f32),
            jax.ShapeDtypeStruct((PAIRS, 8, SEQ), f32), out(16, f32),
        ],
        scratch_shapes=[
            wide, pltpu.VMEM((rows, D), f32), pltpu.VMEM(vector.shape, f32), wide, dma((4,)), dma((6,)),
            full, pltpu.VMEM((SEQ, 3 * D), bf16), full, full, wide, wide, wide, full, full,
            pltpu.VMEM((SEQ, 256), bf16), pltpu.VMEM((SEQ, 256), bf16), pltpu.VMEM((D, D), bf16),
            block, block, dma((4,)), pltpu.VMEM((2, 2, 256, D), bf16), dma((2, 2)),
            pltpu.VMEM((rows, D), bf16), dma,
            pltpu.VMEM((3 * D, D), bf16), dma,
            pltpu.VMEM((16, 128), f32), pltpu.VMEM((na, 16, 128), f32),
            pltpu.VMEM((16, D), bf16), pltpu.VMEM((8, 16, D), bf16), dma((7 + na,)), dma((7 + na,)),
            pltpu.VMEM((SEQ, 128), f32),
            dma((2 * na, FINE)), dma((na, FINE)), dma((na,)), dma((na,)), dma((na,)),
            dma((na, FINE)), dma((na, FINE)),
            dma((na, FINE)), dma((na, FINE)),
            dma((na, FINE)), dma((na, FINE)),
            dma((na, 4, FINE)), dma((na, 4, FINE)),
        ],
        compiler_params=pltpu.CompilerParams(
            collective_id=1, has_side_effects=True, vmem_limit_bytes=66_000_000
        ),
        name="gather_forward",
    )(lengths, tokens, master, vector, cotangent)


def tiles(rows, parts):
    marks = [16 * round(rows * h / parts / 16) for h in range(parts)] + [rows]
    return [(marks[h], marks[h + 1] - marks[h]) for h in range(parts)]


def backward_kernel(
    n_dp, weights, ge, qkv_in, mixed_in, lse, n1_in, low_in, tokens_in, base_in, vec, part,
    gl, out, total, vector_total,
    w_out, w_qkv, qkv, mixed, n1, low, tokens, base, load_sem,
    do, proj, stage, stage_sem, kT, dqT, dk_s, dv_s, dl,
    gbuf, kbuf, dbuf, xbuf, ybuf, zbuf, cbuf, vin, vtmp,
    ls, ks, kr, ds, dr, xs, xr, ys, yr, zs, zr, cs, cr, vs, vr,
):
    me = Place(n_dp)
    na = me.na
    nq = na // 4
    a, b, y, c = me.a, me.b, me.y, me.c
    rows = total.shape[0]
    around = ((b, y), (1 - b, y), (b, 1 - y), (1 - b, 1 - y))
    quarters = tiles(rows, 4)
    early = 3 * D

    def span(q):
        return quarters[2 * q][0], quarters[2 * q][1] + quarters[2 * q + 1][1]

    def grads(a_, o, core, q):
        first, size = span(q)
        at = me.sid(a_, *around[o], core) * rows + first
        if isinstance(a_, int):
            return gl.at[pl.ds(pl.multiple_of(at, 8), size)]
        return ge.at[pl.ds(pl.multiple_of(at - early, 8), size)]

    def fetch(a_, o, q):
        return pltpu.make_async_copy(grads(a_, o, c, q), gbuf.at[a_, o, pl.ds(*span(q))], ls.at[a_, o, q])

    def to_core(a_, o, q):
        return pltpu.make_async_remote_copy(
            src_ref=grads(a_, o, 1 - c, q), dst_ref=kbuf.at[a_, o, pl.ds(*span(q))],
            send_sem=ks.at[a_, o, q], recv_sem=kr.at[a_, o, q], device_id=me.core_mate(),
        )

    def move(src, dst, send, recv, peer):
        return pltpu.make_async_remote_copy(src_ref=src, dst_ref=dst, send_sem=send, recv_sem=recv, device_id=peer)

    def diag(a_, h):
        at = pl.ds(*quarters[h])
        peer = me.x_mate() if h % 2 == 0 else me.y_mate()
        return move(kbuf.at[a_, 3, at], dbuf.at[a_, at], ds.at[a_, h], dr.at[a_, h], peer)

    def x_copy(a_, h):
        at = pl.ds(*quarters[h])
        return move(kbuf.at[a_, 1, at], xbuf.at[a_, at], xs.at[a_, h], xr.at[a_, h], me.x_mate())

    def y_copy(a_, h):
        at = pl.ds(*quarters[h])
        return move(kbuf.at[a_, 2, at], ybuf.at[a_, at], ys.at[a_, h], yr.at[a_, h], me.y_mate())

    def direct(a_, q):
        at = pl.ds(*span(q))
        return move(kbuf.at[a_, 0, at], zbuf.at[a, at], zs.at[a_, q], zr.at[a, q], me.at(a_))

    def direct_from(a_, q):
        at = pl.ds(*span(q))
        return move(kbuf.at[a_, 0, at], zbuf.at[a_, at], zs.at[a_, q], zr.at[a_, q], me.at(a_))

    def chain(a_, h, down):
        at = pl.ds(*quarters[h])
        way = 0 if down else 1
        return move(
            kbuf.at[a_, 0, at], cbuf.at[a_, way, at], cs.at[a_, h], cr.at[a_, way, h], me.at(a - 1 if down else a + 1)
        )

    def add(to, frm):
        kbuf[to] = (kbuf[to].astype(f32) + frm.astype(f32)).astype(bf16)

    def start(a_, q):
        for o in range(4):
            to_core(a_, o, q).start()
            fetch(a_, o, q).start()

    def pair_sum(a_, q):
        at = pl.ds(*span(q))
        for o in (3, 1, 2, 0):
            to_core(a_, o, q).wait_recv()
            fetch(a_, o, q).wait()
            add((a_, o, at), gbuf[a_, o, at])
            if o == 3:
                diag(a_, 2 * q).start()
                diag(a_, 2 * q + 1).start()
            if o == 1:
                x_copy(a_, 2 * q).start()
            if o == 2:
                y_copy(a_, 2 * q + 1).start()

    def diag_sum(a_, q):
        at = pl.ds(*quarters[2 * q])
        diag(a_, 2 * q).wait_recv()
        add((a_, 2, at), dbuf[a_, at])
        y_copy(a_, 2 * q).start()
        at = pl.ds(*quarters[2 * q + 1])
        diag(a_, 2 * q + 1).wait_recv()
        add((a_, 1, at), dbuf[a_, at])
        x_copy(a_, 2 * q + 1).start()

    def plane_sum(a_, h):
        at = pl.ds(*quarters[h])
        x_copy(a_, h).wait_recv()
        y_copy(a_, h).wait_recv()
        add((a_, 0, at), xbuf[a_, at].astype(f32) + ybuf[a_, at].astype(f32))

    def spread(a_, q):
        plane_sum(a_, 2 * q)
        plane_sum(a_, 2 * q + 1)

        @pl.when(a_ != a)
        def _():
            direct(a_, q).start()

    def link(a_, h):
        at = pl.ds(*quarters[h])
        plane_sum(a_, h)

        @pl.when(a > a_)
        def _():
            @pl.when(a + 1 < na)
            def _():
                chain(a_, h, True).wait_recv()
                add((a_, 0, at), cbuf[a_, 0, at])

            chain(a_, h, True).start()

        @pl.when(a < a_)
        def _():
            @pl.when(a > 0)
            def _():
                chain(a_, h, False).wait_recv()
                add((a_, 0, at), cbuf[a_, 1, at])

            chain(a_, h, False).start()

    def item(i):
        return nq + i // 2 + 0 * a, i % 2

    def local(k, src, dst):
        return pltpu.make_async_copy(src, dst, load_sem.at[k])

    loads = [
        local(0, low_in, low), local(1, weights.at[pl.ds(3 * D, D)], w_out), local(2, qkv_in, qkv),
        local(3, mixed_in, mixed), local(4, n1_in, n1), local(5, weights.at[pl.ds(0, 3 * D)], w_qkv),
        local(6, tokens_in, tokens), local(7, base_in, base),
    ]
    for load in loads[:4]:
        load.start()
    greet(me, (me.x_mate(), me.y_mate(), me.core_mate()))

    @pl.loop(nq, na)
    def _(a_):
        for q in range(2):
            start(a_, q)

    for load in loads[4:]:
        load.start()
    loads[0].wait()
    loads[1].wait()

    @pl.loop(0, 3)
    def _(j):
        at = pl.ds(pl.multiple_of(j * 256, 256), 256)
        do[:, at] = dot(low[...], w_out[:, at], NN).astype(bf16)

    pair_sum(*item(0))
    pair_sum(*item(1))
    loads[2].wait()
    loads[3].wait()

    lo = lax.broadcasted_iota(jnp.int32, (1, 128), 1) < 64
    zero = jnp.zeros((), bf16)

    def attend_back(i):
        q_at = pl.ds(pl.multiple_of(i * 128, 128), 128)
        k_at = pl.ds(pl.multiple_of(D + i * 128, 128), 128)
        v_at = pl.ds(pl.multiple_of(2 * D + i * 128, 128), 128)
        prod = do[:, q_at].astype(f32) * mixed[:, q_at].astype(f32)
        d0 = jnp.sum(jnp.where(lo, prod, 0.0), 1, keepdims=True)
        d1 = jnp.sum(jnp.where(lo, 0.0, prod), 1, keepdims=True)
        dl[...] = jnp.transpose(jnp.where(lo, d0, d1), (1, 0))
        kT[...] = jnp.transpose(qkv[:, k_at], (1, 0))
        for qb in range(SEQ // QB):
            q0 = qb * QB
            end = q0 + QB
            for h in range(2):
                offset = lse[i, h:h + 1, q0:end]
                delta = dl[64 * h:64 * h + 1, q0:end]
                qm, dm = qkv[q0:end, q_at], do[q0:end, q_at]
                qm = jnp.where(lo, qm, zero) if h == 0 else jnp.where(lo, zero, qm)
                dm = jnp.where(lo, dm, zero) if h == 0 else jnp.where(lo, zero, dm)
                s = dot(qkv[:end, k_at], qm, NT)
                ki = lax.broadcasted_iota(jnp.int32, (QB, QB), 0)
                qi = lax.broadcasted_iota(jnp.int32, (QB, QB), 1)
                last = jnp.where(ki <= qi, s[q0:], NEG)
                s = jnp.concatenate([s[:q0], last], 0) if qb else last
                p = jnp.exp(s - offset)
                dp = dot(qkv[:end, v_at], dm, NT)
                dsc = (p * (dp - delta)).astype(bf16)
                pv = dot(p.astype(bf16), dm, NN)
                pk = dot(dsc, qm, NN)
                if h == 0:
                    if qb:
                        dv_s[:q0, :] += pv[:q0]
                        dk_s[:q0, :] += pk[:q0]
                    dv_s[q0:end, :] = pv[q0:]
                    dk_s[q0:end, :] = pk[q0:]
                else:
                    dv_s[:end, :] += pv
                    dk_s[:end, :] += pk
                dqT[64 * h:64 * h + 64, q0:end] = dot(kT[64 * h:64 * h + 64, :end], dsc, NN)
        dq = jnp.transpose(dqT[...], (1, 0)) * 0.125
        dv = dv_s[...]
        proj[:, q_at] = dq.astype(bf16)
        proj[:, k_at] = dk_s[...].astype(bf16)
        proj[:, v_at] = dv.astype(bf16)
        vin[0, 2:3, q_at] = jnp.sum(dq, 0, keepdims=True)
        vin[0, 3:4, q_at] = jnp.sum(dv, 0, keepdims=True)

    vin[0] = part[...]
    steps = ((0, diag_sum, 0), (1, pair_sum, 2), (1, diag_sum, 1), (2, spread, 0), (2, pair_sum, 3),
             (3, diag_sum, 2), (3, spread, 1), (4, diag_sum, 3), (5, spread, 2), (5, pair_sum, 4))

    @pl.loop(0, PAIRS)
    def _(i):
        attend_back(i)
        for k, act, which in steps:
            @pl.when(i == k)
            def _():
                act(*item(which))

    loads[4].wait()

    def save(j):
        return pltpu.make_async_copy(
            stage.at[j % 2], gl.at[pl.ds(pl.multiple_of(j * 256, 256), 256)], stage_sem.at[j % 2]
        )

    def start_saved(low_end, high_end):
        for a_ in range(nq):
            for q in range(2):
                first, size = span(q)
                for o in range(4):
                    for core, copy in ((1 - c, to_core), (c, fetch)):
                        end = me.sid(a_, *around[o], core) * rows + first + size

                        @pl.when((end > low_end) & (end <= high_end))
                        def _():
                            copy(a_, o, q).start()

    @pl.loop(0, 9)
    def _(j):
        @pl.when(j >= 2)
        def _():
            save(j - 2).wait()
            start_saved((j - 2) * 256, (j - 1) * 256)

        stage[j % 2] = dot(proj[:, pl.ds(pl.multiple_of(j * 256, 256), 256)], n1[...], TN).astype(bf16)
        save(j).start()

    save(7).wait()
    save(8).wait()
    start_saved(7 * 256, 9 * 256)
    for load in loads[5:]:
        load.wait()

    def norm_back(t):
        at = pl.ds(t * 256, 256)
        x = tokens[at, :]
        centred = x - jnp.mean(x, -1, keepdims=True)
        inverse = lax.rsqrt(jnp.mean(centred * centred, -1, keepdims=True) + EPS)
        unit = centred * inverse
        g = dot(proj[at, :], w_qkv[...], NN)
        e = g * vec[0:1, :]
        out[at, :] = base[at, :] + inverse * (
            e - jnp.mean(e, -1, keepdims=True) - unit * jnp.mean(e * unit, -1, keepdims=True)
        )
        vin[0, 0:1, :] += jnp.sum(g * unit, 0, keepdims=True)
        vin[0, 1:2, :] += jnp.sum(g, 0, keepdims=True)

    def vec_copy(i, k, peer):
        return pltpu.make_async_remote_copy(
            src_ref=vin.at[i], dst_ref=vtmp.at[k], send_sem=vs.at[k], recv_sem=vr.at[k], device_id=peer
        )

    v_core, v_y, v_x = vec_copy(0, 0, me.core_mate()), vec_copy(1, 1, me.y_mate()), vec_copy(2, 2, me.x_mate())

    def vec_at(i):
        return vec_copy(3, 2 + i, me.at((a + i) % na))

    late = [(a_, q) for a_ in range(nq) for q in range(2)]
    norm_back(0)
    diag_sum(*item(4))
    for one in late:
        pair_sum(*one)
    norm_back(1)
    spread(*item(3))
    norm_back(2)
    diag_sum(*late[0])
    norm_back(3)
    v_core.start()
    for one in late[1:]:
        diag_sum(*one)
    pair_sum(*item(5))
    spread(*item(4))
    v_core.wait()
    vin[1] = vin[0] + vtmp[0]
    v_y.start()
    for a_ in range(nq):
        link(a_, 0)
        link(a_, 1)
    diag_sum(*item(5))
    v_y.wait()
    vin[2] = vin[1] + vtmp[1]
    v_x.start()
    for a_ in range(nq):
        link(a_, 2)
        link(a_, 3)
    v_x.wait()
    vin[3] = vin[2] + vtmp[2]
    for i in range(1, na):
        vec_at(i).start()
    spread(*item(5))

    if na > 4:
        @pl.loop(nq + 3, na)
        def _(a_):
            for q in range(2):
                pair_sum(a_, q)
                diag_sum(a_, q)
                spread(a_, q)

    vsum = vin[3]
    for i in range(1, na):
        vec_at(i).wait()
        vsum = vsum + vtmp[2 + i]
    vector_total[...] = vsum

    @pl.when(a >= nq)
    def _():
        total[...] = kbuf[a, 0].astype(f32)

        @pl.loop(1, na)
        def _(i):
            frm = (a + i) % na
            for q in range(2):
                direct_from(frm, q).wait_recv()
            total[...] += zbuf[frm].astype(f32)

    for a_ in range(nq):
        @pl.when(a == a_)
        def _():
            total[...] = kbuf[a_, 0].astype(f32)

            @pl.when(a + 1 < na)
            def _():
                for h in range(4):
                    chain(a_, h, True).wait_recv()
                total[...] += cbuf[a_, 0].astype(f32)

            @pl.when(a > 0)
            def _():
                for h in range(4):
                    chain(a_, h, False).wait_recv()
                total[...] += cbuf[a_, 1].astype(f32)

        @pl.when(a != a_)
        def _():
            for h in range(4):
                chain(a_, h, True).wait_send()

    def sent(a_):
        for q in range(2):
            for o in range(4):
                to_core(a_, o, q).wait_send()
        for h in range(4):
            diag(a_, h).wait_send()
            x_copy(a_, h).wait_send()
            y_copy(a_, h).wait_send()

    for a_ in range(nq):
        sent(a_)

    @pl.loop(nq, na)
    def _(a_):
        sent(a_)

        @pl.when(a_ != a)
        def _():
            for q in range(2):
                direct(a_, q).wait_send()


def backward(n_dp, rows, weights, ge, qkv, mixed, lse, n1, low, tokens, base, vec, part):
    na = n_dp // 2
    nq = na // 4
    dma = pltpu.SemaphoreType.DMA
    vm, anyw = pl.BlockSpec(memory_space=pltpu.VMEM), pl.BlockSpec(memory_space=pl.ANY)
    full = pltpu.VMEM((SEQ, D), bf16)
    wide = pltpu.VMEM((SEQ, D), f32)
    return pl.pallas_call(
        functools.partial(backward_kernel, n_dp),
        in_specs=[anyw, anyw, anyw, anyw, vm, anyw, anyw, anyw, anyw, vm, vm],
        out_specs=[anyw, vm, vm, vm],
        out_shape=[
            jax.ShapeDtypeStruct((3 * D, D), bf16),
            jax.ShapeDtypeStruct((SEQ, D), f32),
            jax.ShapeDtypeStruct((rows, D), f32),
            jax.ShapeDtypeStruct((16, D), f32),
        ],
        scratch_shapes=[
            pltpu.VMEM((D, D), bf16), pltpu.VMEM((3 * D, D), bf16), pltpu.VMEM((SEQ, 3 * D), bf16),
            full, full, full, wide, wide, dma((8,)),
            full, pltpu.VMEM((SEQ, 3 * D), bf16), pltpu.VMEM((2, 256, D), bf16), dma((2,)),
            pltpu.VMEM((128, SEQ), bf16), pltpu.VMEM((128, SEQ), f32),
            pltpu.VMEM((SEQ, 128), f32), pltpu.VMEM((SEQ, 128), f32), pltpu.VMEM((128, SEQ), f32),
            pltpu.VMEM((na, 4, rows, D), bf16), pltpu.VMEM((na, 4, rows, D), bf16),
            pltpu.VMEM((na, rows, D), bf16), pltpu.VMEM((na, rows, D), bf16),
            pltpu.VMEM((na, rows, D), bf16), pltpu.VMEM((na, rows, D), bf16),
            pltpu.VMEM((nq, 2, rows, D), bf16),
            pltpu.VMEM((4, 16, D), f32), pltpu.VMEM((2 + na, 16, D), f32),
            dma((na, 4, 2)), dma((na, 4, 2)), dma((na, 4, 2)),
            dma((na, 4)), dma((na, 4)), dma((na, 4)), dma((na, 4)), dma((na, 4)), dma((na, 4)),
            dma((na, 2)), dma((na, 2)), dma((nq, 4)), dma((nq, 2, 4)), dma((2 + na,)), dma((2 + na,)),
        ],
        compiler_params=pltpu.CompilerParams(
            collective_id=2, has_side_effects=True, vmem_limit_bytes=66_000_000
        ),
        name="attend_reduce",
    )(weights, ge, qkv, mixed, lse, n1, low, tokens, base, vec, part)


BETA_ONE = 0.9
BETA_TWO = 0.95
ADAM_EPS = 1e-08
ADAM_STEP = 2
LR_MATRIX = 0.05
LR_VECTOR = 0.1
DECAY = 0.1
GRAD_FACTOR = 4.0


def adamw(master, gradient, moment, square, rate, decay):
    moment_new = BETA_ONE * moment + (1.0 - BETA_ONE) * gradient
    square_new = BETA_TWO * square + (1.0 - BETA_TWO) * gradient * gradient
    first_fix = 1.0 - BETA_ONE**ADAM_STEP
    second_fix = 1.0 - BETA_TWO**ADAM_STEP
    stride = moment_new / first_fix / (jnp.sqrt(square_new / second_fix) + ADAM_EPS)
    return (master - rate * (stride + decay * master), moment_new, square_new)


def body(
    tokens, cotangent, lengths, master_matrix, master_vector,
    moment_matrix, moment_vector, square_matrix, square_vector,
):
    n_dp, n_zero = lax.axis_size("dp"), lax.axis_size("zero")
    weights, early, normed_one, qkv, mixed, mid_low, base, block_out, vectors, lse, part = forward(
        n_dp, lengths, tokens, master_matrix, master_vector, cotangent
    )
    late, input_gradient, matrix_total, vector_sum = backward(
        n_dp, master_matrix.shape[0], weights, early, qkv, mixed, lse, normed_one, mid_low, tokens, base, vectors, part
    )
    columns = master_vector.shape[1]
    mine = (lax.axis_index("dp") * n_zero + lax.axis_index("zero")) * columns
    vector_total = lax.dynamic_slice(vector_sum, (0, mine), (12, columns))
    scale = GRAD_FACTOR * float(SEQ * n_dp * n_zero) ** (-0.5)
    matrix_gradient = matrix_total * scale
    vector_gradient = vector_total * scale
    matrix_weights, matrix_moment, matrix_square = adamw(
        master_matrix, matrix_gradient, moment_matrix, square_matrix, LR_MATRIX, DECAY
    )
    vector_weights, vector_moment, vector_square = adamw(
        master_vector, vector_gradient, moment_vector, square_vector, LR_VECTOR, 0.0
    )
    return (
        block_out, input_gradient, matrix_gradient, vector_gradient, matrix_weights,
        vector_weights, matrix_moment, vector_moment, matrix_square, vector_square,
    )


def solution(mesh):
    rows, columns = P(("dp", "zero"), None), P(None, ("dp", "zero"))
    return jax.shard_map(
        body,
        mesh=mesh,
        in_specs=(rows, rows, P(("dp", "zero")), rows, columns, rows, columns, rows, columns),
        out_specs=(rows, rows, rows, columns, rows, columns, rows, columns, rows, columns),
        check_vma=False,
    )
```

```python
import functools
import jax, jax.numpy as jnp
from jax import lax
from jax.experimental import pallas as pl
from jax.experimental.pallas import tpu as pltpu
from jax.sharding import PartitionSpec as P

f32, bf16 = jnp.float32, jnp.bfloat16
D = 768
SEQ = 1024
PAIRS = 6
FF = 3072
EPS = 1e-05
NEG = -1e30
CUBIC = 0.044715
ROOT = 0.7978845608028654
QB = 256
NT = (((1,), (1,)), ((), ()))
NN = (((1,), (0,)), ((), ()))
TN = (((0,), (0,)), ((), ()))


def dot(a, b, dn):
    return lax.dot_general(a, b, dn, preferred_element_type=f32)


def cuts(rows, parts):
    marks = [8 * round(rows * h / parts / 8) for h in range(parts + 1)]
    return [(marks[h], marks[h + 1] - marks[h]) for h in range(parts)]


class Place:
    def __init__(self, n_dp):
        self.na = n_dp // 2
        dp, zero = lax.axis_index("dp"), lax.axis_index("zero")
        self.a, self.b, self.y, self.c = dp // 2, dp % 2, zero // 2, zero % 2

    def sid(self, a, b, y, c):
        return ((a * 2 + b) * 2 + y) * 2 + c

    def dev(self, a, b, y, c):
        return {"dp": a * 2 + b, "zero": y * 2 + c}

    def x_mate(self):
        return self.dev(self.a, 1 - self.b, self.y, self.c)

    def y_mate(self):
        return self.dev(self.a, self.b, 1 - self.y, self.c)

    def core_mate(self):
        return self.dev(self.a, self.b, self.y, 1 - self.c)

    def plane_mate(self, r):
        b = 1 - self.b if r & 1 else self.b
        y = 1 - self.y if r & 2 else self.y
        return self.dev(self.a, b, y, 1 - self.c if r & 4 else self.c)

    def at(self, a):
        return self.dev(a, self.b, self.y, self.c)


def greet(me, peers):
    barrier = pltpu.get_barrier_semaphore()
    for peer in peers:
        pl.semaphore_signal(barrier, inc=1, device_id=peer)
    for i in range(1, me.na):
        pl.semaphore_signal(barrier, inc=1, device_id=me.at((me.a + i) % me.na))
    pl.semaphore_wait(barrier, me.na - 1 + len(peers))


FINE = 4
HALVES = 2


def forward_kernel(
    n_dp, lengths, tokens_in, master_in, vector_in, cot_in,
    whole, ge, n1_out, qkv_out, mixed_out, low_out, base_out, block_out, vec, lse, part_sums,
    tokens, master, vector, cot, load_sem, save_sem,
    n1, qkv, mixed, low, after, acc, ngrad, n2, top_low, act, hid, w_out, wf, wd, w_sem, stage, stage_sem,
    own, own_sem, wq, wq_sem, tile, tiles_in, vin, vtmp, vs_sem, vr_sem, lc,
    ch_s, ch_r, up_s, dn_s, ds, xs, xr, ys, yr, fs, fr, ks, kr,
):
    me = Place(n_dp)
    na = me.na
    nq = na // 4
    a, b, y, c = me.a, me.b, me.y, me.c
    rows = master.shape[0]
    relay = na == 4
    around = ((b, y), (1 - b, y), (b, 1 - y), (1 - b, 1 - y))

    def remote(s, h, n, send, recv, peer):
        first, size = cuts(rows, n)[h]
        ref = whole.at[pl.ds(pl.multiple_of(s * rows + first, 8), size)]
        return pltpu.make_async_remote_copy(
            src_ref=ref, dst_ref=ref, send_sem=send, recv_sem=recv, device_id=peer
        )

    def chain_down(a_, h):
        return remote(me.sid(a_, b, y, c), h, FINE, ch_s.at[a_, h], ch_r.at[a_, h], me.at(a - 1))

    def chain_up(a_, h):
        return remote(me.sid(a_, b, y, c), h, FINE, ch_s.at[na + a_, h], ch_r.at[a_, h], me.at(a + 1))

    def direct(to):
        return remote(me.sid(a, b, y, c), 0, 1, ds.at[to], ch_r.at[a, 0], me.at(to))

    def direct_from(a_):
        return remote(me.sid(a_, b, y, c), 0, 1, ds.at[a_], ch_r.at[a_, 0], me.at(a_))

    def x_copy(a_, h, n, mine=True):
        return remote(me.sid(a_, b if mine else 1 - b, y, c), h, n, xs.at[a_, h], xr.at[a_, h], me.x_mate())

    def y_copy(a_, h, n, mine=True):
        return remote(me.sid(a_, b, y if mine else 1 - y, c), h, n, ys.at[a_, h], yr.at[a_, h], me.y_mate())

    def diag_send(a_, h, n):
        if h < n // 2:
            return remote(me.sid(a_, 1 - b, y, c), h, n, fs.at[a_, h], fr.at[a_, h], me.y_mate())
        return remote(me.sid(a_, b, 1 - y, c), h, n, fs.at[a_, h], fr.at[a_, h], me.x_mate())

    def diag_recv(a_, h, n):
        return remote(me.sid(a_, 1 - b, 1 - y, c), h, n, fs.at[a_, h], fr.at[a_, h], me.x_mate())

    def core(a_, b_, y_, h, n, mine=True):
        o = (b_ + b) % 2 + 2 * ((y_ + y) % 2)
        return remote(
            me.sid(a_, b_, y_, c if mine else 1 - c), h, n, ks.at[a_, o, h], kr.at[a_, o, h], me.core_mate()
        )

    def column_sends(a_, h, n):
        x_copy(a_, h, n).start()
        y_copy(a_, h, n).start()
        core(a_, b, y, h, n).start()

    def pass_chain(h):
        for a_ in range(nq):
            @pl.when(a != a_)
            def _():
                chain_up(a_, h).wait_recv()

                @pl.when((a_ < a) & (a + 1 < na))
                def _():
                    chain_up(a_, h).start()

                @pl.when((a_ > a) & (a > 0))
                def _():
                    chain_down(a_, h).start()

                column_sends(a_, h, FINE)

    def relay_up(a_):
        return remote(me.sid(a_, b, y, c), 0, 1, up_s.at[a_], ch_r.at[a_, 0], me.at(a + 1))

    def relay_down(a_):
        return remote(me.sid(a_, b, y, c), 0, 1, dn_s.at[a_], ch_r.at[a_, 0], me.at(a - 1))

    def take(a_):
        direct_from(a_).wait_recv()
        if relay:
            @pl.when((a_ < a) & (a + 1 < na))
            def _():
                relay_up(a_).start()

            @pl.when((a_ > a) & (a > 0))
            def _():
                relay_down(a_).start()

    def share(a_):
        for h in range(HALVES):
            column_sends(a_, h, HALVES)

    def pass_plane(a_, n):
        for h in range(n):
            x_copy(a_, h, n, False).wait_recv()
            if h < n // 2:
                diag_send(a_, h, n).start()
            core(a_, 1 - b, y, h, n).start()
            y_copy(a_, h, n, False).wait_recv()
            if h >= n // 2:
                diag_send(a_, h, n).start()
            core(a_, b, 1 - y, h, n).start()

    def pass_diag(a_, n):
        for h in range(n):
            diag_recv(a_, h, n).wait_recv()
            core(a_, 1 - b, 1 - y, h, n).start()

    def partner(a_, n):
        for b_, y_ in around:
            for h in range(n):
                core(a_, b_, y_, h, n, False).wait_recv()

    def load(k, src, dst):
        return pltpu.make_async_copy(src, dst, load_sem.at[k])

    loads = [load(0, master_in, master), load(1, vector_in, vector), load(2, tokens_in, tokens), load(3, cot_in, cot)]
    for one in loads:
        one.start()
    mine = me.sid(a, b, y, c)
    columns = vector.shape[1]
    loads[0].wait()
    loads[1].wait()
    own[...] = master[...].astype(bf16)
    put = pltpu.make_async_copy(own, whole.at[pl.ds(pl.multiple_of(mine * rows, 8), rows)], own_sem)
    put.start()
    narrow = (
        lax.broadcasted_iota(jnp.int32, (columns, 128), 1) == lax.broadcasted_iota(jnp.int32, (columns, 128), 0)
    ).astype(bf16)
    tile[0:12, :] = dot(vector[...].astype(bf16), narrow, NN)
    tile[12:16, :] = jnp.zeros((4, 128), f32)

    def widen(small, s):
        move = (
            lax.broadcasted_iota(jnp.int32, (128, D), 1) == lax.broadcasted_iota(jnp.int32, (128, D), 0) + s * columns
        ) & (lax.broadcasted_iota(jnp.int32, (128, D), 0) < columns)
        return dot(small.astype(bf16), move.astype(bf16), NN)

    greet(me, [me.plane_mate(r) for r in range(1, 8)])
    put.wait()

    def vec_copy(r):
        return pltpu.make_async_remote_copy(
            src_ref=vin, dst_ref=vtmp.at[r], send_sem=vs_sem.at[r], recv_sem=vr_sem.at[r],
            device_id=me.plane_mate(r),
        )

    def vec_at(i):
        return pltpu.make_async_remote_copy(
            src_ref=tile, dst_ref=tiles_in.at[i], send_sem=vs_sem.at[7 + i], recv_sem=vr_sem.at[7 + i],
            device_id=me.at((a + i) % na),
        )

    for i in range(1, na):
        vec_at(i).start()

    @pl.when(a < nq)
    def _():
        for h in range(FINE):
            @pl.when(a + 1 < na)
            def _():
                chain_up(a, h).start()

            @pl.when(a > 0)
            def _():
                chain_down(a, h).start()

        for h in range(FINE // 2):
            x_copy(a, h, FINE).start()
            y_copy(a, h, FINE).start()

    @pl.when(a >= nq)
    def _():
        x_copy(a, 0, HALVES).start()
        y_copy(a, 0, HALVES).start()
        if relay:
            @pl.when(a > 0)
            def _():
                relay_down(a).start()
        else:
            @pl.loop(1, na)
            def _(d):
                @pl.when(d <= a)
                def _():
                    direct(a - d).start()

    def rest():
        for copy in (x_copy, y_copy):
            copy(a, 1, HALVES).start()

    total = widen(tile[...], mine)
    for i in range(1, na):
        vec_at(i).wait()
        total = total + widen(tiles_in[i], me.sid((a - i + na) % na, b, y, c))
    vin[...] = total.astype(bf16)
    for r in range(1, 8):
        vec_copy(r).start()

    @pl.when(a < nq)
    def _():
        for h in range(FINE // 2, FINE):
            x_copy(a, h, FINE).start()
            y_copy(a, h, FINE).start()

    @pl.when(a > nq if relay else a >= nq)
    def _():
        rest()

    def at_slot(slot):
        for k in range(na if relay else 0):
            acts = plan[k].get(slot, ())

            if acts:
                @pl.when(a == k)
                def _():
                    for act_now, plane in acts:
                        act_now(plane)

    def plane(a_):
        pass_plane(a_, HALVES)

    def diagonal(a_):
        pass_diag(a_, HALVES)

    def partners(a_):
        partner(a_, HALVES)

    plan = (
        {
            "chain": ((take, 1),), "plane": ((share, 1),), "v": ((take, 2), (share, 2)), 1: ((plane, 1),),
            3: ((diagonal, 1),), 4: ((plane, 2), (take, 3), (share, 3)),
            "feed": ((diagonal, 2), (partners, 1), (partners, 2)), "out": ((plane, 3),),
            "all": ((diagonal, 3), (partners, 3)),
        },
        {
            "chain": ((take, 2),), "plane": ((lambda a_: rest(), 1), (share, 2)), "q": ((take, 3),),
            "v": ((plane, 1),), 0: ((share, 3),), 1: ((diagonal, 1),), 2: ((plane, 2),), 4: ((diagonal, 2),),
            5: ((plane, 3),), "feed": ((partners, 1), (partners, 2)), "out": ((diagonal, 3),), "all": ((partners, 3),),
        },
        {
            "middle": ((take, 3),), "chain": ((plane, 2),), "plane": ((share, 3),), "norm": ((take, 1),), "q": ((share, 1),),
            "v": ((diagonal, 2),), 2: ((plane, 3),), 3: ((plane, 1),), 4: ((diagonal, 3),),
            "feed": ((diagonal, 1), (partners, 2), (partners, 1)), "all": ((partners, 3),),
        },
        {
            "middle": ((plane, 3),), "norm": ((take, 2), (share, 2)), "q": ((diagonal, 3), (take, 1), (share, 1)),
            1: ((plane, 2),), 3: ((plane, 1),), 4: ((diagonal, 2),),
            "feed": ((diagonal, 1), (partners, 3), (partners, 2), (partners, 1)),
        },
    )
    pass_chain(0)
    @pl.when(a < nq)
    def _():
        for h in range(FINE):
            core(a, b, y, h, FINE).start()

    @pl.when(a >= nq)
    def _():
        for h in range(HALVES):
            core(a, b, y, h, HALVES).start()

    for h in range(1, FINE):
        pass_chain(h)
        if h == FINE // 2 - 1:
            at_slot("middle")

    @pl.when(a >= nq)
    def _():
        if relay:
            @pl.when(a + 1 < na)
            def _():
                relay_up(a).start()
        else:
            @pl.loop(1, na)
            def _(d):
                @pl.when(a + d < na)
                def _():
                    direct(a + d).start()

    at_slot("chain")
    if not relay:
        @pl.when(a >= nq + 1)
        def _():
            pass_plane(a, HALVES)

    for a_ in range(nq):
        pass_plane(a_, FINE)
    at_slot("plane")
    vec_total = vin[...].astype(f32)
    for r in range(1, 8):
        vec_copy(r).wait()
        vec_total = vec_total + vtmp[r].astype(f32)
    vec[...] = vec_total
    loads[2].wait()

    @pl.loop(0, SEQ // 256)
    def _(t):
        at = pl.ds(pl.multiple_of(t * 256, 256), 256)
        x = tokens[at, :]
        centred = x - jnp.mean(x, -1, keepdims=True)
        inverse = lax.rsqrt(jnp.mean(centred * centred, -1, keepdims=True) + EPS)
        n1[at, :] = (centred * inverse * vec[0:1, :] + vec[1:2, :]).astype(bf16)

    if not relay:
        @pl.when(a == nq)
        def _():
            pass_plane(a, HALVES)

    at_slot("norm")
    for a_ in range(nq):
        pass_diag(a_, FINE)
    for a_ in range(nq):
        partner(a_, FINE)
    fetch_q = pltpu.make_async_copy(whole.at[pl.ds(0, 3 * D)], wq, wq_sem)
    fetch_q.start()

    def save(k, src, dst):
        return pltpu.make_async_copy(src, dst, save_sem.at[k])

    save(0, n1, n1_out).start()
    fetch_q.wait()

    def project(begin, row, scale):
        @pl.loop(begin, begin + 3)
        def _(j):
            at = pl.ds(pl.multiple_of(j * 256, 256), 256)
            r = dot(n1[...], wq[at, :], NT)
            if row is not None:
                cols = pl.ds(pl.multiple_of((j - begin) * 256, 256), 256)
                r = r + vec[row:row + 1, cols]
            r = r.astype(bf16)
            if scale is not None:
                r = r * jnp.asarray(scale, bf16)
            qkv[:, at] = r

    project(0, 2, 0.125)
    at_slot("q")
    project(3, None, None)
    project(6, 3, None)
    at_slot("v")
    save(1, qkv, qkv_out).start()

    lo = lax.broadcasted_iota(jnp.int32, (1, 128), 1) < 64
    zero = jnp.zeros((), bf16)

    def attend(i):
        q_at = pl.ds(pl.multiple_of(i * 128, 128), 128)
        k_at = pl.ds(pl.multiple_of(D + i * 128, 128), 128)
        v_at = pl.ds(pl.multiple_of(2 * D + i * 128, 128), 128)
        for qb in range(SEQ // QB):
            span = (qb + 1) * QB
            outs, sums = [], []
            for h in range(2):
                block = qkv[qb * QB:span, q_at]
                block = jnp.where(lo, block, zero) if h == 0 else jnp.where(lo, zero, block)
                s = dot(block, qkv[:span, k_at], NT)
                qi = lax.broadcasted_iota(jnp.int32, (QB, QB), 0)
                ki = lax.broadcasted_iota(jnp.int32, (QB, QB), 1)
                diag = jnp.where(ki <= qi, s[:, span - QB:], NEG)
                s = jnp.concatenate([s[:, :span - QB], diag], 1) if qb else diag
                m = jnp.max(s, 1, keepdims=True)
                p = jnp.exp(s - m)
                l = jnp.sum(p, 1, keepdims=True)
                outs.append(dot(p.astype(bf16), qkv[:span, v_at], NN) / l)
                sums.append(m + jnp.log(l))
            mixed[qb * QB:span, q_at] = jnp.where(lo, outs[0], outs[1]).astype(bf16)
            lc[qb * QB:span, :] = jnp.where(lo, sums[0], sums[1])
        t = jnp.transpose(lc[...], (1, 0))
        lse[i, 0:1, :] = t[0:1]
        lse[i, 1:2, :] = t[64:65]

    @pl.loop(0, PAIRS)
    def _(i):
        attend(i)
        for k in range(PAIRS):
            if relay:
                @pl.when(i == k)
                def _():
                    at_slot(k)

    save(2, mixed, mixed_out).start()
    at_slot("feed")
    if not relay:
        @pl.when(a >= nq)
        def _():
            pass_diag(a, HALVES)

        for k in range(1, na):
            for a_ in (a + k, a - k):
                @pl.when((a_ >= nq) & (a_ < na))
                def _():
                    take(a_)
                    share(a_)
                    pass_plane(a_, HALVES)
                    pass_diag(a_, HALVES)

        @pl.loop(nq, na)
        def _(a_):
            partner(a_, HALVES)

    fetch_o = pltpu.make_async_copy(whole.at[pl.ds(3 * D, D)], w_out, wq_sem)
    fetch_o.start()
    BLOCKS = FF // 256

    def weights_in(j):
        at = j * 256
        slot = j % 2
        return (
            pltpu.make_async_copy(whole.at[pl.ds(pl.multiple_of(4 * D + at, 256), 256)], wf.at[slot], w_sem.at[slot]),
            pltpu.make_async_copy(
                whole.at[pl.ds(pl.multiple_of(4 * D + FF + at, 256), 256)], wd.at[slot], w_sem.at[2 + slot]
            ),
        )

    for one in weights_in(0):
        one.start()
    loads[3].wait()
    fetch_o.wait()
    length = lengths[0]

    def alive(t):
        return lax.broadcasted_iota(jnp.int32, (256, 1), 0) + t * 256 < length

    @pl.loop(0, SEQ // 256)
    def _(t):
        at = pl.ds(pl.multiple_of(t * 256, 256), 256)
        x = tokens[at, :] + dot(mixed[at, :], w_out[...], NT) + vec[4:5, :]
        after[at, :] = x
        centred = x - jnp.mean(x, -1, keepdims=True)
        inverse = lax.rsqrt(jnp.mean(centred * centred, -1, keepdims=True) + EPS)
        n2[at, :] = (centred * inverse * vec[5:6, :] + vec[6:7, :]).astype(bf16)
        acc[at, :] = x + vec[7:8, :]
        top_low[at, :] = jnp.where(alive(t), cot[at, :], 0.0).astype(bf16)
        ngrad[at, :] = jnp.zeros((256, D), f32)

    at_slot("out")

    def put_grad(k, slot, row):
        return pltpu.make_async_copy(
            stage.at[slot, k], ge.at[pl.ds(pl.multiple_of(row, 256), 256)], stage_sem.at[slot, k]
        )

    def put_both(j):
        at = j * 256
        return put_grad(0, j % 2, D + at), put_grad(1, j % 2, D + FF + at)

    @pl.loop(0, BLOCKS)
    def _(j):
        @pl.when(j == 2)
        def _():
            at_slot("all")

        @pl.when(j + 1 < BLOCKS)
        def _():
            for one in weights_in(j + 1):
                one.start()

        for one in weights_in(j):
            one.wait()
        slot = j % 2
        unit = j
        line, cols = 8 + unit // 3, pl.ds(pl.multiple_of(unit % 3 * 256, 256), 256)
        bias = vec[pl.ds(line, 1), cols]
        sums = jnp.zeros((1, 256), f32)
        for t in range(SEQ // 256):
            at = pl.ds(t * 256, 256)
            x = dot(n2[at, :], wf[slot], NT) + bias
            g = dot(top_low[at, :], wd[slot], NT)
            square = x * x
            part = 0.5 + 0.5 * jnp.tanh(ROOT * x * (1.0 + CUBIC * square))
            active = (x * part).astype(bf16)
            slope = part * (1.0 + (2.0 * ROOT) * x * (1.0 - part) * (1.0 + (3.0 * CUBIC) * square))
            g = g * slope
            sums = sums + jnp.sum(g, 0, keepdims=True)
            g = g.astype(bf16)
            act[at, :] = active
            hid[at, :] = g
            acc[at, :] += dot(active, wd[slot], NN)
            ngrad[at, :] += dot(g, wf[slot], NN)
        part_sums[pl.ds(line, 1), cols] = sums

        @pl.when(j >= 2)
        def _():
            for one in put_both(j - 2):
                one.wait()

        stage[slot, 0] = dot(hid[...], n2[...], TN).astype(bf16)
        stage[slot, 1] = dot(act[...], top_low[...], TN).astype(bf16)
        for one in put_both(j):
            one.start()

    part_sums[0:8, :] = jnp.zeros((8, D), f32)
    part_sums[12:16, :] = jnp.zeros((4, D), f32)

    @pl.loop(0, SEQ // 256)
    def _(t):
        at = pl.ds(pl.multiple_of(t * 256, 256), 256)
        live = alive(t)
        x = after[at, :]
        centred = x - jnp.mean(x, -1, keepdims=True)
        inverse = lax.rsqrt(jnp.mean(centred * centred, -1, keepdims=True) + EPS)
        unit = centred * inverse
        g = ngrad[at, :]
        e = g * vec[5:6, :]
        top = jnp.where(live, cot[at, :], 0.0)
        mid = top + inverse * (e - jnp.mean(e, -1, keepdims=True) - unit * jnp.mean(e * unit, -1, keepdims=True))
        low[at, :] = mid.astype(bf16)
        part_sums[4:5, :] += jnp.sum(mid, 0, keepdims=True)
        part_sums[5:6, :] += jnp.sum(g * unit, 0, keepdims=True)
        part_sums[6:7, :] += jnp.sum(g, 0, keepdims=True)
        part_sums[7:8, :] += jnp.sum(top, 0, keepdims=True)
        ngrad[at, :] = mid + jnp.where(live, 0.0, cot[at, :])
        acc[at, :] = jnp.where(live, acc[at, :], tokens[at, :])

    finals = [save(3, low, low_out), save(4, ngrad, base_out), save(5, acc, block_out)]
    for one in finals:
        one.start()
    for j in (BLOCKS - 2, BLOCKS - 1):
        for one in put_both(j):
            one.wait()

    @pl.loop(0, 3)
    def _(j):
        @pl.when(j >= 2)
        def _():
            put_grad(0, 0, 0).wait()

        stage[j % 2, 0] = dot(low[:, pl.ds(pl.multiple_of(j * 256, 256), 256)], mixed[...], TN).astype(bf16)
        put_grad(0, j % 2, j * 256).start()

    put_grad(0, 1, 256).wait()
    put_grad(0, 0, 512).wait()
    for one in [save(0, n1, n1_out), save(1, qkv, qkv_out), save(2, mixed, mixed_out)] + finals:
        one.wait()

    def sent(a_, n):
        for h in range(n):
            x_copy(a_, h, n).wait_send()
            y_copy(a_, h, n).wait_send()
            diag_send(a_, h, n).wait_send()
            for b_, y_ in around:
                core(a_, b_, y_, h, n).wait_send()

    for a_ in range(nq):
        sent(a_, FINE)
        for h in range(FINE):
            @pl.when((a_ <= a) & (a + 1 < na))
            def _():
                chain_up(a_, h).wait_send()

            @pl.when((a_ >= a) & (a > 0))
            def _():
                chain_down(a_, h).wait_send()

    @pl.loop(nq, na)
    def _(a_):
        sent(a_, HALVES)

    if relay:
        @pl.loop(nq, na)
        def _(a_):
            @pl.when((a_ <= a) & (a + 1 < na))
            def _():
                relay_up(a_).wait_send()

            @pl.when((a_ >= a) & (a > 0))
            def _():
                relay_down(a_).wait_send()
    else:
        @pl.when(a >= nq)
        def _():
            @pl.loop(0, na)
            def _(to):
                @pl.when(to != a)
                def _():
                    direct(to).wait_send()


def forward(n_dp, lengths, tokens, master, vector, cotangent):
    na = n_dp // 2
    rows = master.shape[0]
    count = na * 8
    dma = pltpu.SemaphoreType.DMA
    vm, hbm = pl.BlockSpec(memory_space=pltpu.VMEM), pl.BlockSpec(memory_space=pl.ANY)
    wide, full = pltpu.VMEM((SEQ, D), f32), pltpu.VMEM((SEQ, D), bf16)
    block = pltpu.VMEM((2, 256, D), bf16)

    def out(rows, dtype, columns=D):
        return jax.ShapeDtypeStruct((rows, columns), dtype)

    return pl.pallas_call(
        functools.partial(forward_kernel, n_dp),
        in_specs=[pl.BlockSpec(memory_space=pltpu.SMEM), hbm, hbm, hbm, hbm],
        out_specs=[hbm] * 8 + [vm, vm, vm],
        out_shape=[
            out(count * rows, bf16), out(count * rows - 3 * D, bf16), out(SEQ, bf16), out(SEQ, bf16, 3 * D),
            out(SEQ, bf16), out(SEQ, bf16), out(SEQ, f32), out(SEQ, f32), out(16, f32),
            jax.ShapeDtypeStruct((PAIRS, 8, SEQ), f32), out(16, f32),
        ],
        scratch_shapes=[
            wide, pltpu.VMEM((rows, D), f32), pltpu.VMEM(vector.shape, f32), wide, dma((4,)), dma((6,)),
            full, pltpu.VMEM((SEQ, 3 * D), bf16), full, full, wide, wide, wide, full, full,
            pltpu.VMEM((SEQ, 256), bf16), pltpu.VMEM((SEQ, 256), bf16), pltpu.VMEM((D, D), bf16),
            block, block, dma((4,)), pltpu.VMEM((2, 2, 256, D), bf16), dma((2, 2)),
            pltpu.VMEM((rows, D), bf16), dma,
            pltpu.VMEM((3 * D, D), bf16), dma,
            pltpu.VMEM((16, 128), f32), pltpu.VMEM((na, 16, 128), f32),
            pltpu.VMEM((16, D), bf16), pltpu.VMEM((8, 16, D), bf16), dma((7 + na,)), dma((7 + na,)),
            pltpu.VMEM((SEQ, 128), f32),
            dma((2 * na, FINE)), dma((na, FINE)), dma((na,)), dma((na,)), dma((na,)),
            dma((na, FINE)), dma((na, FINE)),
            dma((na, FINE)), dma((na, FINE)),
            dma((na, FINE)), dma((na, FINE)),
            dma((na, 4, FINE)), dma((na, 4, FINE)),
        ],
        compiler_params=pltpu.CompilerParams(
            collective_id=1, has_side_effects=True, vmem_limit_bytes=66_000_000
        ),
        name="gather_forward",
    )(lengths, tokens, master, vector, cotangent)


def tiles(rows, parts):
    marks = [16 * round(rows * h / parts / 16) for h in range(parts)] + [rows]
    return [(marks[h], marks[h + 1] - marks[h]) for h in range(parts)]


def backward_kernel(
    n_dp, weights, ge, qkv_in, mixed_in, lse, n1_in, low_in, tokens_in, base_in, vec, part,
    gl, out, total, vector_total,
    w_out, w_qkv, qkv, mixed, n1, low, tokens, base, load_sem,
    do, proj, stage, stage_sem, kT, dqT, dk_s, dv_s, dl,
    gbuf, kbuf, dbuf, xbuf, ybuf, zbuf, cbuf, vin, vtmp,
    ls, ks, kr, ds, dr, xs, xr, ys, yr, zs, zr, cs, cr, vs, vr,
):
    me = Place(n_dp)
    na = me.na
    nq = na // 4
    a, b, y, c = me.a, me.b, me.y, me.c
    rows = total.shape[0]
    around = ((b, y), (1 - b, y), (b, 1 - y), (1 - b, 1 - y))
    quarters = tiles(rows, 4)
    early = 3 * D

    def span(q):
        return quarters[2 * q][0], quarters[2 * q][1] + quarters[2 * q + 1][1]

    def grads(a_, o, core, q):
        first, size = span(q)
        at = me.sid(a_, *around[o], core) * rows + first
        if isinstance(a_, int):
            return gl.at[pl.ds(pl.multiple_of(at, 8), size)]
        return ge.at[pl.ds(pl.multiple_of(at - early, 8), size)]

    def fetch(a_, o, q):
        return pltpu.make_async_copy(grads(a_, o, c, q), gbuf.at[a_, o, pl.ds(*span(q))], ls.at[a_, o, q])

    def to_core(a_, o, q):
        return pltpu.make_async_remote_copy(
            src_ref=grads(a_, o, 1 - c, q), dst_ref=kbuf.at[a_, o, pl.ds(*span(q))],
            send_sem=ks.at[a_, o, q], recv_sem=kr.at[a_, o, q], device_id=me.core_mate(),
        )

    def move(src, dst, send, recv, peer):
        return pltpu.make_async_remote_copy(src_ref=src, dst_ref=dst, send_sem=send, recv_sem=recv, device_id=peer)

    def diag(a_, h):
        at = pl.ds(*quarters[h])
        peer = me.x_mate() if h % 2 == 0 else me.y_mate()
        return move(kbuf.at[a_, 3, at], dbuf.at[a_, at], ds.at[a_, h], dr.at[a_, h], peer)

    def x_copy(a_, h):
        at = pl.ds(*quarters[h])
        return move(kbuf.at[a_, 1, at], xbuf.at[a_, at], xs.at[a_, h], xr.at[a_, h], me.x_mate())

    def y_copy(a_, h):
        at = pl.ds(*quarters[h])
        return move(kbuf.at[a_, 2, at], ybuf.at[a_, at], ys.at[a_, h], yr.at[a_, h], me.y_mate())

    def direct(a_, q):
        at = pl.ds(*span(q))
        return move(kbuf.at[a_, 0, at], zbuf.at[a, at], zs.at[a_, q], zr.at[a, q], me.at(a_))

    def direct_from(a_, q):
        at = pl.ds(*span(q))
        return move(kbuf.at[a_, 0, at], zbuf.at[a_, at], zs.at[a_, q], zr.at[a_, q], me.at(a_))

    def chain(a_, h, down):
        at = pl.ds(*quarters[h])
        way = 0 if down else 1
        return move(
            kbuf.at[a_, 0, at], cbuf.at[a_, way, at], cs.at[a_, h], cr.at[a_, way, h], me.at(a - 1 if down else a + 1)
        )

    def add(to, frm):
        kbuf[to] = (kbuf[to].astype(f32) + frm.astype(f32)).astype(bf16)

    def start(a_, q):
        for o in range(4):
            to_core(a_, o, q).start()
            fetch(a_, o, q).start()

    def pair_sum(a_, q):
        at = pl.ds(*span(q))
        for o in (3, 1, 2, 0):
            to_core(a_, o, q).wait_recv()
            fetch(a_, o, q).wait()
            add((a_, o, at), gbuf[a_, o, at])
            if o == 3:
                diag(a_, 2 * q).start()
                diag(a_, 2 * q + 1).start()
            if o == 1:
                x_copy(a_, 2 * q).start()
            if o == 2:
                y_copy(a_, 2 * q + 1).start()

    def diag_sum(a_, q):
        at = pl.ds(*quarters[2 * q])
        diag(a_, 2 * q).wait_recv()
        add((a_, 2, at), dbuf[a_, at])
        y_copy(a_, 2 * q).start()
        at = pl.ds(*quarters[2 * q + 1])
        diag(a_, 2 * q + 1).wait_recv()
        add((a_, 1, at), dbuf[a_, at])
        x_copy(a_, 2 * q + 1).start()

    def plane_sum(a_, h):
        at = pl.ds(*quarters[h])
        x_copy(a_, h).wait_recv()
        y_copy(a_, h).wait_recv()
        add((a_, 0, at), xbuf[a_, at].astype(f32) + ybuf[a_, at].astype(f32))

    def spread(a_, q):
        plane_sum(a_, 2 * q)
        plane_sum(a_, 2 * q + 1)

        @pl.when(a_ != a)
        def _():
            direct(a_, q).start()

    def link(a_, h):
        at = pl.ds(*quarters[h])
        plane_sum(a_, h)

        @pl.when(a > a_)
        def _():
            @pl.when(a + 1 < na)
            def _():
                chain(a_, h, True).wait_recv()
                add((a_, 0, at), cbuf[a_, 0, at])

            chain(a_, h, True).start()

        @pl.when(a < a_)
        def _():
            @pl.when(a > 0)
            def _():
                chain(a_, h, False).wait_recv()
                add((a_, 0, at), cbuf[a_, 1, at])

            chain(a_, h, False).start()

    def item(i):
        return nq + (i // 2 + 2) % 3 + 0 * a, i % 2

    def local(k, src, dst):
        return pltpu.make_async_copy(src, dst, load_sem.at[k])

    loads = [
        local(0, low_in, low), local(1, weights.at[pl.ds(3 * D, D)], w_out), local(2, qkv_in, qkv),
        local(3, mixed_in, mixed), local(4, n1_in, n1), local(5, weights.at[pl.ds(0, 3 * D)], w_qkv),
        local(6, tokens_in, tokens), local(7, base_in, base),
    ]
    for load in loads[:4]:
        load.start()
    greet(me, (me.x_mate(), me.y_mate(), me.core_mate()))

    @pl.loop(nq, na)
    def _(a_):
        for q in range(2):
            start(a_, q)

    for load in loads[4:]:
        load.start()
    loads[0].wait()
    loads[1].wait()

    @pl.loop(0, 3)
    def _(j):
        at = pl.ds(pl.multiple_of(j * 256, 256), 256)
        do[:, at] = dot(low[...], w_out[:, at], NN).astype(bf16)

    pair_sum(*item(0))
    pair_sum(*item(1))
    loads[2].wait()
    loads[3].wait()

    lo = lax.broadcasted_iota(jnp.int32, (1, 128), 1) < 64
    zero = jnp.zeros((), bf16)

    def attend_back(i):
        q_at = pl.ds(pl.multiple_of(i * 128, 128), 128)
        k_at = pl.ds(pl.multiple_of(D + i * 128, 128), 128)
        v_at = pl.ds(pl.multiple_of(2 * D + i * 128, 128), 128)
        prod = do[:, q_at].astype(f32) * mixed[:, q_at].astype(f32)
        d0 = jnp.sum(jnp.where(lo, prod, 0.0), 1, keepdims=True)
        d1 = jnp.sum(jnp.where(lo, 0.0, prod), 1, keepdims=True)
        dl[...] = jnp.transpose(jnp.where(lo, d0, d1), (1, 0))
        kT[...] = jnp.transpose(qkv[:, k_at], (1, 0))
        for qb in range(SEQ // QB):
            q0 = qb * QB
            end = q0 + QB
            for h in range(2):
                offset = lse[i, h:h + 1, q0:end]
                delta = dl[64 * h:64 * h + 1, q0:end]
                qm, dm = qkv[q0:end, q_at], do[q0:end, q_at]
                qm = jnp.where(lo, qm, zero) if h == 0 else jnp.where(lo, zero, qm)
                dm = jnp.where(lo, dm, zero) if h == 0 else jnp.where(lo, zero, dm)
                s = dot(qkv[:end, k_at], qm, NT)
                ki = lax.broadcasted_iota(jnp.int32, (QB, QB), 0)
                qi = lax.broadcasted_iota(jnp.int32, (QB, QB), 1)
                last = jnp.where(ki <= qi, s[q0:], NEG)
                s = jnp.concatenate([s[:q0], last], 0) if qb else last
                p = jnp.exp(s - offset)
                dp = dot(qkv[:end, v_at], dm, NT)
                dsc = (p * (dp - delta)).astype(bf16)
                pv = dot(p.astype(bf16), dm, NN)
                pk = dot(dsc, qm, NN)
                if h == 0:
                    if qb:
                        dv_s[:q0, :] += pv[:q0]
                        dk_s[:q0, :] += pk[:q0]
                    dv_s[q0:end, :] = pv[q0:]
                    dk_s[q0:end, :] = pk[q0:]
                else:
                    dv_s[:end, :] += pv
                    dk_s[:end, :] += pk
                dqT[64 * h:64 * h + 64, q0:end] = dot(kT[64 * h:64 * h + 64, :end], dsc, NN)
        dq = jnp.transpose(dqT[...], (1, 0)) * 0.125
        dv = dv_s[...]
        proj[:, q_at] = dq.astype(bf16)
        proj[:, k_at] = dk_s[...].astype(bf16)
        proj[:, v_at] = dv.astype(bf16)
        vin[0, 2:3, q_at] = jnp.sum(dq, 0, keepdims=True)
        vin[0, 3:4, q_at] = jnp.sum(dv, 0, keepdims=True)

    vin[0] = part[...]
    steps = ((0, diag_sum, 0), (1, pair_sum, 2), (1, diag_sum, 1), (2, spread, 0), (2, pair_sum, 3),
             (3, diag_sum, 2), (3, spread, 1), (4, diag_sum, 3), (5, spread, 2), (5, pair_sum, 4))

    @pl.loop(0, PAIRS)
    def _(i):
        attend_back(i)
        for k, act, which in steps:
            @pl.when(i == k)
            def _():
                act(*item(which))

    loads[4].wait()
    pair_sum(*item(5))

    def save(j):
        return pltpu.make_async_copy(
            stage.at[j % 2], gl.at[pl.ds(pl.multiple_of(j * 256, 256), 256)], stage_sem.at[j % 2]
        )

    def start_saved(low_end, high_end):
        for a_ in range(nq):
            for q in range(2):
                first, size = span(q)
                for o in range(4):
                    for core, copy in ((1 - c, to_core), (c, fetch)):
                        end = me.sid(a_, *around[o], core) * rows + first + size

                        @pl.when((end > low_end) & (end <= high_end))
                        def _():
                            copy(a_, o, q).start()

    @pl.loop(0, 9)
    def _(j):
        @pl.when(j >= 2)
        def _():
            save(j - 2).wait()
            start_saved((j - 2) * 256, (j - 1) * 256)

        stage[j % 2] = dot(proj[:, pl.ds(pl.multiple_of(j * 256, 256), 256)], n1[...], TN).astype(bf16)
        save(j).start()

    save(7).wait()
    save(8).wait()
    start_saved(7 * 256, 9 * 256)
    for load in loads[5:]:
        load.wait()

    def norm_back(t):
        at = pl.ds(t * 256, 256)
        x = tokens[at, :]
        centred = x - jnp.mean(x, -1, keepdims=True)
        inverse = lax.rsqrt(jnp.mean(centred * centred, -1, keepdims=True) + EPS)
        unit = centred * inverse
        g = dot(proj[at, :], w_qkv[...], NN)
        e = g * vec[0:1, :]
        out[at, :] = base[at, :] + inverse * (
            e - jnp.mean(e, -1, keepdims=True) - unit * jnp.mean(e * unit, -1, keepdims=True)
        )
        vin[0, 0:1, :] += jnp.sum(g * unit, 0, keepdims=True)
        vin[0, 1:2, :] += jnp.sum(g, 0, keepdims=True)

    def vec_copy(i, k, peer):
        return pltpu.make_async_remote_copy(
            src_ref=vin.at[i], dst_ref=vtmp.at[k], send_sem=vs.at[k], recv_sem=vr.at[k], device_id=peer
        )

    v_core, v_y, v_x = vec_copy(0, 0, me.core_mate()), vec_copy(1, 1, me.y_mate()), vec_copy(2, 2, me.x_mate())

    def vec_at(i):
        return vec_copy(3, 2 + i, me.at((a + i) % na))

    late = [(a_, q) for a_ in range(nq) for q in range(2)]
    norm_back(0)
    diag_sum(*item(4))
    for one in late:
        pair_sum(*one)
    norm_back(1)
    spread(*item(3))
    norm_back(2)
    diag_sum(*late[0])
    norm_back(3)
    v_core.start()
    for one in late[1:]:
        diag_sum(*one)
    spread(*item(4))
    v_core.wait()
    vin[1] = vin[0] + vtmp[0]
    v_y.start()
    diag_sum(*item(5))
    for a_ in range(nq):
        link(a_, 0)
        link(a_, 1)
    v_y.wait()
    vin[2] = vin[1] + vtmp[1]
    v_x.start()
    for a_ in range(nq):
        link(a_, 2)
        link(a_, 3)
    v_x.wait()
    vin[3] = vin[2] + vtmp[2]
    for i in range(1, na):
        vec_at(i).start()
    spread(*item(5))

    if na > 4:
        @pl.loop(nq + 3, na)
        def _(a_):
            for q in range(2):
                pair_sum(a_, q)
                diag_sum(a_, q)
                spread(a_, q)

    vsum = vin[3]
    for i in range(1, na):
        vec_at(i).wait()
        vsum = vsum + vtmp[2 + i]
    vector_total[...] = vsum

    @pl.when(a >= nq)
    def _():
        total[...] = kbuf[a, 0].astype(f32)

        @pl.loop(1, na)
        def _(i):
            frm = (a + i) % na
            for q in range(2):
                direct_from(frm, q).wait_recv()
            total[...] += zbuf[frm].astype(f32)

    for a_ in range(nq):
        @pl.when(a == a_)
        def _():
            total[...] = kbuf[a_, 0].astype(f32)

            @pl.when(a + 1 < na)
            def _():
                for h in range(4):
                    chain(a_, h, True).wait_recv()
                total[...] += cbuf[a_, 0].astype(f32)

            @pl.when(a > 0)
            def _():
                for h in range(4):
                    chain(a_, h, False).wait_recv()
                total[...] += cbuf[a_, 1].astype(f32)

        @pl.when(a != a_)
        def _():
            for h in range(4):
                chain(a_, h, True).wait_send()

    def sent(a_):
        for q in range(2):
            for o in range(4):
                to_core(a_, o, q).wait_send()
        for h in range(4):
            diag(a_, h).wait_send()
            x_copy(a_, h).wait_send()
            y_copy(a_, h).wait_send()

    for a_ in range(nq):
        sent(a_)

    @pl.loop(nq, na)
    def _(a_):
        sent(a_)

        @pl.when(a_ != a)
        def _():
            for q in range(2):
                direct(a_, q).wait_send()


def backward(n_dp, rows, weights, ge, qkv, mixed, lse, n1, low, tokens, base, vec, part):
    na = n_dp // 2
    nq = na // 4
    dma = pltpu.SemaphoreType.DMA
    vm, anyw = pl.BlockSpec(memory_space=pltpu.VMEM), pl.BlockSpec(memory_space=pl.ANY)
    full = pltpu.VMEM((SEQ, D), bf16)
    wide = pltpu.VMEM((SEQ, D), f32)
    return pl.pallas_call(
        functools.partial(backward_kernel, n_dp),
        in_specs=[anyw, anyw, anyw, anyw, vm, anyw, anyw, anyw, anyw, vm, vm],
        out_specs=[anyw, vm, vm, vm],
        out_shape=[
            jax.ShapeDtypeStruct((3 * D, D), bf16),
            jax.ShapeDtypeStruct((SEQ, D), f32),
            jax.ShapeDtypeStruct((rows, D), f32),
            jax.ShapeDtypeStruct((16, D), f32),
        ],
        scratch_shapes=[
            pltpu.VMEM((D, D), bf16), pltpu.VMEM((3 * D, D), bf16), pltpu.VMEM((SEQ, 3 * D), bf16),
            full, full, full, wide, wide, dma((8,)),
            full, pltpu.VMEM((SEQ, 3 * D), bf16), pltpu.VMEM((2, 256, D), bf16), dma((2,)),
            pltpu.VMEM((128, SEQ), bf16), pltpu.VMEM((128, SEQ), f32),
            pltpu.VMEM((SEQ, 128), f32), pltpu.VMEM((SEQ, 128), f32), pltpu.VMEM((128, SEQ), f32),
            pltpu.VMEM((na, 4, rows, D), bf16), pltpu.VMEM((na, 4, rows, D), bf16),
            pltpu.VMEM((na, rows, D), bf16), pltpu.VMEM((na, rows, D), bf16),
            pltpu.VMEM((na, rows, D), bf16), pltpu.VMEM((na, rows, D), bf16),
            pltpu.VMEM((nq, 2, rows, D), bf16),
            pltpu.VMEM((4, 16, D), f32), pltpu.VMEM((2 + na, 16, D), f32),
            dma((na, 4, 2)), dma((na, 4, 2)), dma((na, 4, 2)),
            dma((na, 4)), dma((na, 4)), dma((na, 4)), dma((na, 4)), dma((na, 4)), dma((na, 4)),
            dma((na, 2)), dma((na, 2)), dma((nq, 4)), dma((nq, 2, 4)), dma((2 + na,)), dma((2 + na,)),
        ],
        compiler_params=pltpu.CompilerParams(
            collective_id=2, has_side_effects=True, vmem_limit_bytes=66_000_000
        ),
        name="attend_reduce",
    )(weights, ge, qkv, mixed, lse, n1, low, tokens, base, vec, part)


BETA_ONE = 0.9
BETA_TWO = 0.95
ADAM_EPS = 1e-08
ADAM_STEP = 2
LR_MATRIX = 0.05
LR_VECTOR = 0.1
DECAY = 0.1
GRAD_FACTOR = 4.0


def adamw(master, gradient, moment, square, rate, decay):
    moment_new = BETA_ONE * moment + (1.0 - BETA_ONE) * gradient
    square_new = BETA_TWO * square + (1.0 - BETA_TWO) * gradient * gradient
    first_fix = 1.0 - BETA_ONE**ADAM_STEP
    second_fix = 1.0 - BETA_TWO**ADAM_STEP
    stride = moment_new / first_fix / (jnp.sqrt(square_new / second_fix) + ADAM_EPS)
    return (master - rate * (stride + decay * master), moment_new, square_new)


def body(
    tokens, cotangent, lengths, master_matrix, master_vector,
    moment_matrix, moment_vector, square_matrix, square_vector,
):
    n_dp, n_zero = lax.axis_size("dp"), lax.axis_size("zero")
    weights, early, normed_one, qkv, mixed, mid_low, base, block_out, vectors, lse, part = forward(
        n_dp, lengths, tokens, master_matrix, master_vector, cotangent
    )
    late, input_gradient, matrix_total, vector_sum = backward(
        n_dp, master_matrix.shape[0], weights, early, qkv, mixed, lse, normed_one, mid_low, tokens, base, vectors, part
    )
    columns = master_vector.shape[1]
    mine = (lax.axis_index("dp") * n_zero + lax.axis_index("zero")) * columns
    vector_total = lax.dynamic_slice(vector_sum, (0, mine), (12, columns))
    scale = GRAD_FACTOR * float(SEQ * n_dp * n_zero) ** (-0.5)
    matrix_gradient = matrix_total * scale
    vector_gradient = vector_total * scale
    matrix_weights, matrix_moment, matrix_square = adamw(
        master_matrix, matrix_gradient, moment_matrix, square_matrix, LR_MATRIX, DECAY
    )
    vector_weights, vector_moment, vector_square = adamw(
        master_vector, vector_gradient, moment_vector, square_vector, LR_VECTOR, 0.0
    )
    return (
        block_out, input_gradient, matrix_gradient, vector_gradient, matrix_weights,
        vector_weights, matrix_moment, vector_moment, matrix_square, vector_square,
    )


def solution(mesh):
    rows, columns = P(("dp", "zero"), None), P(None, ("dp", "zero"))
    return jax.shard_map(
        body,
        mesh=mesh,
        in_specs=(rows, rows, P(("dp", "zero")), rows, columns, rows, columns, rows, columns),
        out_specs=(rows, rows, rows, columns, rows, columns, rows, columns, rows, columns),
        check_vma=False,
    )
```
